8 devices in a mesh: rhs: 1 (over z), mz: 2 (over y), my: 2 (over x), mx: 2 (over core).
Axes of the slice: x: 2, y: 2, z: 1, core: 2. Of those that a mesh axis runs over, the one named last changes fastest.
Arguments:
- x_vol: bfloat16 [128, 128, 128, 64], P('mx', 'my', 'mz', 'rhs')
- fac_a1: bfloat16 [32, 128], replicated
- fac_a2: bfloat16 [32, 128], replicated
- fac_a3: bfloat16 [32, 128], replicated
- diag_d: float32 [32, 32, 32], P('mx', 'my', 'mz')
- fac_b1: bfloat16 [128, 32], replicated
- fac_b2: bfloat16 [128, 32], replicated
- fac_b3: bfloat16 [128, 32], replicated
Outputs:
- output: float32 [128, 128, 128, 64], P('mx', 'my', 'mz', 'rhs')
All inputs are finite; a program needn't handle non-finite values.
Results may differ from the reference program's by a relative error of at most 0.0125944.
Values are sent between devices in bfloat16 or wider.
A program may use at most 1 GiB of HBM per device.

```python
import jax
import jax.numpy as jnp

N1 = 128
N2 = 128
N3 = 128
C = 64
M1 = N1 // 4
M2 = N2 // 4
M3 = N3 // 4


def setup_inputs(seed: int = 0, part: int = 0) -> dict:
    base_key = jax.random.key(seed)
    key_list = jax.random.split(base_key, 8)
    vol_key = jax.random.fold_in(key_list[0], part)
    x_vol = jax.random.normal(vol_key, (N1, N2, N3, C), jnp.float32).astype(jnp.bfloat16)
    fac_a1 = (jax.random.normal(key_list[1], (M1, N1), jnp.float32) * N1 ** -0.5).astype(jnp.bfloat16)
    fac_a2 = (jax.random.normal(key_list[2], (M2, N2), jnp.float32) * N2 ** -0.5).astype(jnp.bfloat16)
    fac_a3 = (jax.random.normal(key_list[3], (M3, N3), jnp.float32) * N3 ** -0.5).astype(jnp.bfloat16)
    diag_d = jnp.exp(jax.random.uniform(key_list[4], (M1, M2, M3), jnp.float32, -1.15, 1.15))
    fac_b1 = (jax.random.normal(key_list[5], (N1, M1), jnp.float32) * M1 ** -0.5).astype(jnp.bfloat16)
    fac_b2 = (jax.random.normal(key_list[6], (N2, M2), jnp.float32) * M2 ** -0.5).astype(jnp.bfloat16)
    fac_b3 = (jax.random.normal(key_list[7], (N3, M3), jnp.float32) * M3 ** -0.5).astype(jnp.bfloat16)
    return {"x_vol": x_vol, "fac_a1": fac_a1, "fac_a2": fac_a2, "fac_a3": fac_a3, "diag_d": diag_d, "fac_b1": fac_b1, "fac_b2": fac_b2, "fac_b3": fac_b3}


def mode_product(matrix, tensor, form):
    return jnp.einsum(form, matrix.astype(jnp.float32), tensor.astype(jnp.float32))


def reference(x_vol, fac_a1, fac_a2, fac_a3, diag_d, fac_b1, fac_b2, fac_b3):
    u_one = mode_product(fac_a1, x_vol, "ia,ajkr->ijkr").astype(jnp.bfloat16)
    u_two = mode_product(fac_a2, u_one, "jb,ibkr->ijkr").astype(jnp.bfloat16)
    u_three = mode_product(fac_a3, u_two, "kc,ijcr->ijkr").astype(jnp.bfloat16)
    w_core = (diag_d[:, :, :, None] * u_three.astype(jnp.float32)).astype(jnp.bfloat16)
    v_three = mode_product(fac_b3, w_core, "kc,ijcr->ijkr").astype(jnp.bfloat16)
    v_two = mode_product(fac_b2, v_three, "jb,ibkr->ijkr").astype(jnp.bfloat16)
    return mode_product(fac_b1, v_two, "ia,ajkr->ijkr")
```

```python
import jax
import jax.numpy as jnp
from jax import lax
from jax.experimental import pallas as pl
from jax.experimental.pallas import tpu as pltpu
from jax.sharding import PartitionSpec as P

F32 = jnp.float32
BF16 = jnp.bfloat16
MESH = pl.DeviceIdType.MESH
N = 64
M = 32
L = 128
T = 16
S = 8
TWO = 2
QUART = 4
H = M // TWO
RING = 8
AHEAD = 4
NEAR = 4
STEPS = N // TWO
EARLY = 10
A, B, C, D, E = range(5)
SIZES = (4, 6, 3, 2, 1)
STARTS = (0, 4, 10, 13, 15)
CHUNKS = (0, 0, 4, 2, 1)
GROUPS = range(len(SIZES))
OTHERS = range(1, QUART)
DEVICES = range(1, S)
KINDS = 7
LIMIT = 62 * 1024 * 1024


def dot(a, b):
    return jnp.dot(a, b, preferred_element_type=F32)


def dot_t(a, b):
    return lax.dot_general(a, b, (((0,), (0,)), ((), ())), preferred_element_type=F32)


def iota(shape, axis):
    return lax.broadcasted_iota(jnp.int32, shape, axis)


def ones_where(cond):
    return jnp.where(cond, 1.0, 0.0).astype(BF16)


def fill(out_ref, mat, row_of, col_of, keep, product=dot):
    rows, cols = out_ref.shape
    depth = mat.shape[1] if product is dot else mat.shape[0]
    wide = product(mat, ones_where(iota((depth, cols), 0) == col_of(iota((depth, cols), 1)))).astype(BF16)
    for r0 in range(0, rows, L):
        p = iota((L, wide.shape[0]), 0) + r0
        block = dot(ones_where(iota((L, wide.shape[0]), 1) == row_of(p)), wide)
        same = keep(iota((L, cols), 0) + r0, iota((L, cols), 1))
        out_ref[r0:r0 + L, :] = jnp.where(same, block, 0.0).astype(BF16)


def alike(n):
    return lambda p, q: lax.rem(p, n) == lax.rem(q, n)


def compress_body(x_hbm, a1_ref, a2_ref, a3_ref, b2_ref, b3_ref, d_ref, v2_out,
                  xl, xr, u1o, u1s, u1r, k1o, k1r, k2o, k2r, k3, l3, l2, u2s, u2b, wbuf, dall, v3, v2s,
                  near_sem, xs_sem, xr_sem, credit, us_sem, ur_sem, gs_sem, gr_sem,
                  vs_sem, vr_sem, ws_sem, wr_sem, ds_sem, dr_sem, out_sem):
    c = lax.axis_index("mx")
    y = lax.axis_index("my")
    z = lax.axis_index("mz")
    oc, oy, oz = 1 - c, 1 - y, 1 - z

    def flip(rel):
        return (lax.rem(c + rel // QUART, TWO), lax.rem(y + rel // TWO % TWO, TWO), lax.rem(z + rel % TWO, TWO))

    def beside(rel):
        return (lax.rem(c + rel // TWO, TWO), y, lax.rem(z + rel % TWO, TWO))

    def ids(dev):
        return dict(zip(("mx", "my", "mz"), dev))

    def send(src, dst, s_sem, r_sem, dev):
        return pltpu.make_async_remote_copy(src, dst, s_sem, r_sem, device_id=ids(dev), device_id_type=MESH)

    peer, in_x, in_y = (oc, y, z), (c, oy, z), (c, y, oz)

    barrier = pltpu.get_barrier_semaphore()
    for rel in DEVICES:
        pl.semaphore_signal(barrier, inc=1, device_id=ids(flip(rel)), device_id_type=MESH)
    pl.semaphore_wait(barrier, len(DEVICES))

    def half_of(core, t):
        return x_hbm.at[:, pl.ds(TWO * t, TWO), pl.ds(core * M, M), :]

    def near(t):
        slot = lax.rem(t, NEAR)
        return pltpu.make_async_copy(half_of(c, t), xl.at[slot], near_sem.at[slot])

    def cross(t):
        slot = lax.rem(t, RING)
        return send(half_of(oc, t), xr.at[slot], xs_sem.at[slot], xr_sem.at[slot], peer)

    for t in range(AHEAD):
        cross(t).start()
    for t in range(NEAR - 1):
        near(t).start()

    def slot_of(dev):
        return QUART * dev[0] + TWO * dev[1] + dev[2]

    my_slot = slot_of((c, y, z))

    def diag(rel):
        return send(d_ref, dall.at[my_slot], ds_sem.at[rel - 1], dr_sem.at[rel - 1], flip(rel))

    for rel in DEVICES:
        diag(rel).start()
    dall[my_slot] = d_ref[...]

    def rows_one(p):
        return lax.rem(p // T + H * y, M)

    fill(k1o, a1_ref[...], rows_one, lambda q: c * N + q // T, alike(T))
    fill(k1r, a1_ref[...], rows_one, lambda q: oc * N + q // T, alike(T))

    def pack(ref, slot):
        parts = [jnp.concatenate([ref[slot, :, s, 0:T, :], ref[slot, :, s, T:M, :]], axis=-1).reshape(N * T, L)
                 for s in range(TWO)]
        return jnp.concatenate(parts, axis=1)

    def early(t):
        part = (pl.ds(TWO * t, TWO), pl.ds(0, EARLY * T))
        return send(u1s.at[part], u1r.at[part], us_sem.at[t], ur_sem.at[t], in_x)

    def late(g, n):
        span = N // CHUNKS[g]
        part = (pl.ds(span * n, span), pl.ds(STARTS[g] * T, SIZES[g] * T))
        return send(u1s.at[part], u1r.at[part], gs_sem.at[g, n], gr_sem.at[g, n], in_x)

    @pl.loop(0, STEPS)
    def _(t):
        @pl.when(t + NEAR - 1 < STEPS)
        def _():
            near(t + NEAR - 1).start()

        @pl.when(t >= 1)
        def _():
            early(t - 1).start()

        near(t).wait()
        cross(t).wait_recv()
        acc = dot(k1o[...], pack(xl, lax.rem(t, NEAR))) + dot(k1r[...], pack(xr, lax.rem(t, RING)))
        u1 = acc.astype(BF16)
        for s in range(TWO):
            u1o[TWO * t + s] = u1[:H * T, s * L:(s + 1) * L]
            u1s[TWO * t + s] = u1[H * T:, s * L:(s + 1) * L]

        @pl.when(t < STEPS - RING)
        def _():
            pl.semaphore_signal(credit, inc=1, device_id=ids(peer), device_id_type=MESH)

        @pl.when(t + AHEAD >= RING)
        def _():
            cross(t + AHEAD - RING).wait_send()

        @pl.when((t + AHEAD >= RING) & (t + AHEAD < STEPS))
        def _():
            pl.semaphore_wait(credit, 1)

        @pl.when(t + AHEAD < STEPS)
        def _():
            cross(t + AHEAD).start()

    def depart(g):
        for n in range(CHUNKS[g]):
            late(g, n).start()

    early(STEPS - 1).start()
    depart(C)
    for t in range(STEPS - RING + AHEAD, STEPS):
        cross(t).wait_send()

    fill(k2o, a2_ref[...], lambda p: p // T, lambda q: y * N + q // T, alike(T))
    fill(k2r, a2_ref[...], lambda p: p // T, lambda q: oy * N + q // T, alike(T))
    q = iota((L, N), 1)
    k_first = lax.rem(z + q // T % TWO, TWO) * N + lax.rem(c + q // M, TWO) * M + lax.rem(q, T)
    for half in range(TWO):
        sel = ones_where(iota((L, N), 0) == k_first + T * half)
        k3[half * M:(half + 1) * M, :] = dot(a3_ref[...], sel).astype(BF16)
    fill(l2, b2_ref[...], lambda p: y * N + p // S, lambda q: q // S, alike(S), dot_t)
    fill(l3, b3_ref[...], lambda p: z * N + p // L * T + lax.rem(p, T), lambda q: lax.rem(q, M),
         lambda p, q: lax.rem(p, L) // T == q // M, dot_t)

    def second(i, width):
        def side(ref):
            return jnp.concatenate(
                [ref[:, pl.ds(pl.multiple_of((i + s) * T, T), T), :].reshape(N * T, L) for s in range(width)], axis=1)

        out = dot(k2o[...], side(u1o)) + dot(k2r[...], side(u1r))
        for s in range(width):
            u2s[i + s] = out[:, s * L:(s + 1) * L].astype(BF16)

    def quarter(dev):
        return TWO * dev[0] + dev[2]

    mine = quarter((c, y, z))

    def inner(g, rel):
        dev = beside(rel)
        i_span = pl.ds(STARTS[g], SIZES[g])
        return send(u2s.at[i_span, pl.ds(quarter(dev) * L, L)], u2b.at[rel - 1, i_span],
                    vs_sem.at[g, rel], vr_sem.at[g, rel], dev)

    def all_second(g):
        if SIZES[g] >= TWO:
            @pl.loop(0, SIZES[g] // TWO)
            def _(n):
                second(STARTS[g] + TWO * n, TWO)
        if SIZES[g] % TWO:
            second(STARTS[g] + SIZES[g] - 1, 1)
        for rel in (1, QUART - 1, TWO):
            inner(g, rel).start()

    low = iota((M, L), 1) < N
    lane = iota((M, TWO * L), 1)

    def third(g):
        for rel in OTHERS:
            inner(g, rel).wait_recv()
        base = slot_of((y, c, 0))
        d = jnp.concatenate([dall[base], dall[base + 1]], axis=0)

        @pl.loop(0, SIZES[g] * QUART, unroll=QUART)
        def _(n):
            i = STARTS[g] + n // QUART
            jl = lax.rem(n, QUART)

            def column(s):
                row = pl.multiple_of((TWO * jl + s) * T, T)
                own = u2s[i, pl.ds(pl.multiple_of(mine * L + row, T), T), :]
                return jnp.concatenate([own] + [u2b[rel - 1, i, pl.ds(row, T), :] for rel in OTHERS], axis=0)

            out = dot(k3[...], jnp.concatenate([column(0), column(1)], axis=1))
            first, other = out[:M], out[M:]
            u3 = jnp.where(low, first[:, :L] + pltpu.roll(other[:, :L], N, 1),
                           pltpu.roll(first[:, L:], N, 1) + other[:, L:])
            at = i * T + S * z + TWO * jl
            even = jnp.sum(jnp.where(lane == at, d, 0.0), axis=1, keepdims=True)
            odd = jnp.sum(jnp.where(lane == at + 1, d, 0.0), axis=1, keepdims=True)
            w = jnp.where(low, even, odd) * u3.astype(BF16).astype(F32)
            wbuf[y * H + i, mine * QUART + jl] = w.astype(BF16)

    def share(g, kind, owner, dev):
        at = (pl.ds(owner[1] * H + STARTS[g], SIZES[g]), pl.ds(quarter(owner) * QUART, QUART))
        return send(wbuf.at[at], wbuf.at[at], ws_sem.at[g, kind], wr_sem.at[g, kind], dev)

    OWN_X, OWN_Y, OWN_P, X_Y, X_P, Y_P, D_P = range(KINDS)
    diagonal = (c, oy, oz)

    def gather_first(g):
        for kind, dev in ((OWN_X, in_x), (OWN_Y, in_y), (OWN_P, peer)):
            share(g, kind, (c, y, z), dev).start()

    def gather_rest(g):
        share(g, OWN_X, in_x, in_x).wait_recv()
        share(g, X_Y, in_x, in_y).start()
        share(g, X_P, in_x, peer).start()
        share(g, OWN_Y, in_y, in_y).wait_recv()
        share(g, Y_P, in_y, peer).start()
        share(g, X_Y, diagonal, in_y).wait_recv()
        share(g, D_P, diagonal, peer).start()

    def gather_end(g):
        for kind, owner in ((OWN_P, (c, y, z)), (X_P, in_x), (Y_P, in_y), (D_P, diagonal)):
            share(g, kind, (oc,) + owner[1:], peer).wait_recv()

    low_v = iota((QUART, S, S, L), TWO + 1) < N

    def out_copy(p):
        slot = lax.rem(p, TWO)
        return pltpu.make_async_copy(
            v2s.at[slot], v2_out.at[:, :, pl.ds(pl.multiple_of(p * T, T), T), :], out_sem.at[slot])

    def middle(p):
        @pl.when(p >= TWO)
        def _():
            out_copy(p - TWO).wait()

        slot = lax.rem(p, TWO)
        for jo in range(TWO):
            rhs = jnp.concatenate(
                [wbuf[p + H * s, jo * S:(jo + 1) * S].reshape(TWO * L, L) for s in range(TWO)], axis=1)
            out = dot(l3[...], rhs)
            for s in range(TWO):
                o = out[:, s * L:(s + 1) * L].reshape(QUART, S, TWO, S, L)
                t0, t1 = o[:, :, 0], o[:, :, 1]
                even = jnp.where(low_v, t0, pltpu.roll(t1, N, TWO + 1))
                odd = jnp.where(low_v, pltpu.roll(t0, N, TWO + 1), t1)
                both = jnp.concatenate([even, odd], axis=TWO).astype(BF16)
                v3[:, s, jo * L:(jo + 1) * L, :] = both.reshape(QUART, L, L)
        for kb in range(QUART):
            out = dot(l2[...], jnp.concatenate([v3[kb, 0], v3[kb, 1]], axis=1))
            pair = jnp.concatenate([out[:, :L].reshape(N, S, L), out[:, L:].reshape(N, S, L)], axis=1)
            v2s[slot, kb] = pair.astype(BF16)
        out_copy(p).start()

    def all_middle(g):
        @pl.loop(STARTS[g], STARTS[g] + SIZES[g])
        def _(p):
            middle(p)

    def arrived(g):
        for n in range(CHUNKS[g]):
            late(g, n).wait_recv()

    @pl.loop(0, STEPS)
    def _(t):
        early(t).wait_recv()

    for rel in DEVICES:
        diag(rel).wait_recv()
    all_second(A)
    all_second(B)
    third(A)
    gather_first(A)
    depart(D)
    third(B)
    gather_first(B)
    arrived(C)
    all_second(C)
    gather_rest(A)
    third(C)
    gather_first(C)
    depart(E)
    gather_end(A)
    all_middle(A)
    arrived(D)
    all_second(D)
    gather_rest(B)
    third(D)
    gather_first(D)
    gather_rest(C)
    gather_end(B)
    all_middle(B)
    arrived(E)
    all_second(E)
    gather_end(C)
    all_middle(C)
    third(E)
    gather_first(E)
    gather_rest(D)
    gather_end(D)
    all_middle(D)
    gather_rest(E)
    gather_end(E)
    all_middle(E)

    @pl.loop(0, STEPS)
    def _(t):
        early(t).wait_send()

    for rel in DEVICES:
        diag(rel).wait_send()
    for g in GROUPS:
        for n in range(CHUNKS[g]):
            late(g, n).wait_send()
        for rel in OTHERS:
            inner(g, rel).wait_send()
        for kind in range(KINDS):
            share(g, kind, (c, y, z), peer).wait_send()
    out_copy(H - TWO).wait()
    out_copy(H - 1).wait()


def compress(x, a1, a2, a3, b2_t, b3_t, d):
    vmem = pl.BlockSpec(memory_space=pltpu.VMEM)
    hbm = pl.BlockSpec(memory_space=pl.ANY)
    dma = pltpu.SemaphoreType.DMA
    d_flat = d.transpose(2, 0, 1).reshape(H, H * H)
    u1 = pltpu.VMEM((N, H * T, L), BF16)
    spread = pltpu.VMEM((M * T, N * T), BF16)
    groups = len(SIZES)
    return pl.pallas_call(
        compress_body,
        out_shape=jax.ShapeDtypeStruct((QUART, N, M * S, L), BF16),
        in_specs=[hbm] + [vmem] * 6,
        out_specs=hbm,
        scratch_shapes=[
            pltpu.VMEM((NEAR, N, TWO, M, N), BF16), pltpu.VMEM((RING, N, TWO, M, N), BF16), u1, u1, u1,
            spread, spread, spread, spread, pltpu.VMEM((N, N), BF16),
            pltpu.VMEM((M * T, M * S), BF16), pltpu.VMEM((N * S, M * S), BF16),
            pltpu.VMEM((H, M * T, L), BF16), pltpu.VMEM((len(OTHERS), H, L, L), BF16),
            pltpu.VMEM((M, H, M, L), BF16), pltpu.VMEM((S, H, H * H), F32),
            pltpu.VMEM((QUART, TWO, M * S, L), BF16), pltpu.VMEM((TWO, QUART, N, T, L), BF16),
            dma((NEAR,)), dma((RING,)), dma((RING,)), pltpu.SemaphoreType.REGULAR,
            dma((STEPS,)), dma((STEPS,)), dma((groups, QUART)), dma((groups, QUART)),
            dma((groups, QUART)), dma((groups, QUART)), dma((groups, KINDS)), dma((groups, KINDS)),
            dma((KINDS,)), dma((KINDS,)), dma((TWO,)),
        ],
        compiler_params=pltpu.CompilerParams(collective_id=0, has_side_effects=True, vmem_limit_bytes=LIMIT),
        name="compress",
    )(x, a1, a2, a3, b2_t, b3_t, d_flat)


def expand_body(v2_ref, b1_ref, z_ref, l1):
    @pl.when((pl.program_id(0) == 0) & (pl.program_id(1) == 0))
    def _():
        c = lax.axis_index("mx")
        fill(l1, b1_ref[...], lambda p: c * N + p // S, lambda q: lax.rem(q // S, TWO) * H + q // T, alike(S), dot_t)

    for j in range(0, z_ref.shape[1], TWO):
        out = dot(l1[...], jnp.concatenate([v2_ref[0, j], v2_ref[0, j + 1]], axis=1))
        for s in range(TWO):
            o = out[:, s * L:(s + 1) * L].reshape(N, S, L)
            z_ref[:, j + s, :S, :] = o[:, :, :N]
            z_ref[:, j + s, S:, :] = pltpu.roll(o, N, TWO)[:, :, :N]


def expand(v2, b1_t):
    return pl.pallas_call(
        expand_body,
        grid=(QUART, N // S),
        out_shape=jax.ShapeDtypeStruct((N, N, N, N), F32),
        in_specs=[pl.BlockSpec((1, S, M * S, L), lambda kb, jb: (kb, jb, 0, 0)),
                  pl.BlockSpec((M, L), lambda kb, jb: (0, 0))],
        out_specs=pl.BlockSpec((N, S, T, N), lambda kb, jb: (0, jb, kb, 0)),
        scratch_shapes=[pltpu.VMEM((N * S, M * S), BF16)],
        compiler_params=pltpu.CompilerParams(vmem_limit_bytes=LIMIT),
        name="expand",
    )(v2, b1_t)


def solution(mesh):
    vol_spec = P("mx", "my", "mz", "rhs")
    core_spec = P("mx", "my", "mz")
    full_spec = P()

    def local_operator(x_blk, fac_a1, fac_a2, fac_a3, diag_blk, fac_b1, fac_b2, fac_b3):
        v2 = compress(x_blk, fac_a1, fac_a2, fac_a3, fac_b2.T, fac_b3.T, diag_blk)
        return expand(v2, fac_b1.T)

    return jax.shard_map(local_operator, mesh=mesh, in_specs=(vol_spec, full_spec, full_spec, full_spec, core_spec, full_spec, full_spec, full_spec), out_specs=vol_spec, check_vma=False)
```

```python
import jax
import jax.numpy as jnp
from jax import lax
from jax.experimental import pallas as pl
from jax.experimental.pallas import tpu as pltpu
from jax.sharding import PartitionSpec as P

F32 = jnp.float32
BF16 = jnp.bfloat16
MESH = pl.DeviceIdType.MESH
N = 64
M = 32
L = 128
T = 16
S = 8
TWO = 2
QUART = 4
H = M // TWO
RING = 8
AHEAD = 4
NEAR = 4
STEPS = N // TWO
EARLY = 8
A, B, C, D, E, G = range(6)
SIZES = (4, 4, 4, 2, 1, 1)
STARTS = (0, 4, 8, 12, 14, 15)
CHUNKS = (0, 0, 4, 2, 1, 1)
FILLER = 8
GROUPS = range(len(SIZES))
OTHERS = range(1, QUART)
DEVICES = range(1, S)
KINDS = 7
LIMIT = 62 * 1024 * 1024


def dot(a, b):
    return jnp.dot(a, b, preferred_element_type=F32)


def dot_t(a, b):
    return lax.dot_general(a, b, (((0,), (0,)), ((), ())), preferred_element_type=F32)


def iota(shape, axis):
    return lax.broadcasted_iota(jnp.int32, shape, axis)


def ones_where(cond):
    return jnp.where(cond, 1.0, 0.0).astype(BF16)


def fill(out_ref, mat, row_of, col_of, keep, product=dot):
    rows, cols = out_ref.shape
    depth = mat.shape[1] if product is dot else mat.shape[0]
    wide = product(mat, ones_where(iota((depth, cols), 0) == col_of(iota((depth, cols), 1)))).astype(BF16)
    for r0 in range(0, rows, L):
        p = iota((L, wide.shape[0]), 0) + r0
        block = dot(ones_where(iota((L, wide.shape[0]), 1) == row_of(p)), wide)
        same = keep(iota((L, cols), 0) + r0, iota((L, cols), 1))
        out_ref[r0:r0 + L, :] = jnp.where(same, block, 0.0).astype(BF16)


def alike(n):
    return lambda p, q: lax.rem(p, n) == lax.rem(q, n)


def compress_body(x_hbm, a1_ref, a2_ref, a3_ref, b2_ref, b3_ref, d_ref, v2_out,
                  xl, xr, u1o, u1s, u1r, k1o, k1r, k2o, k2r, k3, l3, l2, u2s, u2b, wbuf, dall, v3, v2s,
                  near_sem, xs_sem, xr_sem, credit, us_sem, ur_sem, gs_sem, gr_sem,
                  vs_sem, vr_sem, ws_sem, wr_sem, ds_sem, dr_sem, out_sem):
    c = lax.axis_index("mx")
    y = lax.axis_index("my")
    z = lax.axis_index("mz")
    oc, oy, oz = 1 - c, 1 - y, 1 - z

    def flip(rel):
        return (lax.rem(c + rel // QUART, TWO), lax.rem(y + rel // TWO % TWO, TWO), lax.rem(z + rel % TWO, TWO))

    def beside(rel):
        return (lax.rem(c + rel // TWO, TWO), y, lax.rem(z + rel % TWO, TWO))

    def ids(dev):
        return dict(zip(("mx", "my", "mz"), dev))

    def send(src, dst, s_sem, r_sem, dev):
        return pltpu.make_async_remote_copy(src, dst, s_sem, r_sem, device_id=ids(dev), device_id_type=MESH)

    peer, in_x, in_y, diagonal = (oc, y, z), (c, oy, z), (c, y, oz), (c, oy, oz)

    barrier = pltpu.get_barrier_semaphore()
    for rel in DEVICES:
        pl.semaphore_signal(barrier, inc=1, device_id=ids(flip(rel)), device_id_type=MESH)

    def half_of(core, t):
        return x_hbm.at[:, pl.ds(TWO * t, TWO), pl.ds(core * M, M), :]

    def near(t):
        slot = lax.rem(t, NEAR)
        return pltpu.make_async_copy(half_of(c, t), xl.at[slot], near_sem.at[slot])

    def cross(t):
        slot = lax.rem(t, RING)
        return send(half_of(oc, t), xr.at[slot], xs_sem.at[slot], xr_sem.at[slot], peer)

    for t in range(NEAR - 1):
        near(t).start()

    def slot_of(dev):
        return QUART * dev[0] + TWO * dev[1] + dev[2]

    dall[slot_of((c, y, z))] = d_ref[...].reshape(H * H, H).T

    def rows_one(p):
        return lax.rem(p // T + H * y, M)

    fill(k1o, a1_ref[...], rows_one, lambda q: c * N + q // T, alike(T))
    fill(k1r, a1_ref[...], rows_one, lambda q: oc * N + q // T, alike(T))
    pl.semaphore_wait(barrier, len(DEVICES))
    for t in range(AHEAD):
        cross(t).start()

    my_slot = slot_of((c, y, z))

    def diag(rel):
        return send(dall.at[my_slot], dall.at[my_slot], ds_sem.at[rel - 1], dr_sem.at[rel - 1], flip(rel))

    for rel in DEVICES:
        diag(rel).start()

    def pack(ref, slot):
        parts = [jnp.concatenate([ref[slot, :, s, 0:T, :], ref[slot, :, s, T:M, :]], axis=-1).reshape(N * T, L)
                 for s in range(TWO)]
        return jnp.concatenate(parts, axis=1)

    def early(t):
        part = (pl.ds(TWO * t, TWO), pl.ds(0, EARLY * T))
        return send(u1s.at[part], u1r.at[part], us_sem.at[t], ur_sem.at[t], in_x)

    def late(g, n):
        span = N // CHUNKS[g]
        part = (pl.ds(span * n, span), pl.ds(STARTS[g] * T, SIZES[g] * T))
        return send(u1s.at[part], u1r.at[part], gs_sem.at[g, n], gr_sem.at[g, n], in_x)

    @pl.loop(0, STEPS)
    def _(t):
        @pl.when(t + NEAR - 1 < STEPS)
        def _():
            near(t + NEAR - 1).start()

        @pl.when(t >= 1)
        def _():
            early(t - 1).start()

        @pl.when(t == 2 * FILLER + 1)
        def _():
            late(C, 0).start()

        near(t).wait()
        cross(t).wait_recv()
        acc = dot(k1o[...], pack(xl, lax.rem(t, NEAR))) + dot(k1r[...], pack(xr, lax.rem(t, RING)))
        u1 = acc.astype(BF16)
        for s in range(TWO):
            u1o[TWO * t + s] = u1[:H * T, s * L:(s + 1) * L]
            u1s[TWO * t + s] = u1[H * T:, s * L:(s + 1) * L]

        @pl.when(t < STEPS - RING)
        def _():
            pl.semaphore_signal(credit, inc=1, device_id=ids(peer), device_id_type=MESH)

        @pl.when(t + AHEAD >= RING)
        def _():
            cross(t + AHEAD - RING).wait_send()

        @pl.when((t + AHEAD >= RING) & (t + AHEAD < STEPS))
        def _():
            pl.semaphore_wait(credit, 1)

        @pl.when(t + AHEAD < STEPS)
        def _():
            cross(t + AHEAD).start()

    def depart(g, first=0):
        for n in range(first, CHUNKS[g]):
            late(g, n).start()

    early(STEPS - 1).start()
    depart(C, 1)
    for t in range(STEPS - RING + AHEAD, STEPS):
        cross(t).wait_send()

    fill(k2o, a2_ref[...], lambda p: p // T, lambda q: y * N + q // T, alike(T))
    fill(k2r, a2_ref[...], lambda p: p // T, lambda q: oy * N + q // T, alike(T))
    q = iota((L, N), 1)
    k_first = lax.rem(z + q // T % TWO, TWO) * N + lax.rem(c + q // M, TWO) * M + lax.rem(q, T)
    for half in range(TWO):
        sel = ones_where(iota((L, N), 0) == k_first + T * half)
        k3[half * M:(half + 1) * M, :] = dot(a3_ref[...], sel).astype(BF16)
    fill(l2, b2_ref[...], lambda p: y * N + p // S, lambda q: q // S, alike(S), dot_t)
    fill(l3, b3_ref[...], lambda p: z * N + p // L * T + lax.rem(p, T), lambda q: lax.rem(q, M),
         lambda p, q: lax.rem(p, L) // T == q // M, dot_t)

    def second(i, width):
        def side(ref):
            return jnp.concatenate(
                [ref[:, pl.ds(pl.multiple_of((i + s) * T, T), T), :].reshape(N * T, L) for s in range(width)], axis=1)

        out = dot(k2o[...], side(u1o)) + dot(k2r[...], side(u1r))
        for s in range(width):
            u2s[i + s] = out[:, s * L:(s + 1) * L].astype(BF16)

    def quarter(dev):
        return TWO * dev[0] + dev[2]

    mine = quarter((c, y, z))

    def inner(g, rel):
        dev = beside(rel)
        i_span = pl.ds(STARTS[g], SIZES[g])
        return send(u2s.at[i_span, pl.ds(quarter(dev) * L, L)], u2b.at[rel - 1, i_span],
                    vs_sem.at[g, rel], vr_sem.at[g, rel], dev)

    def all_second(g):
        if SIZES[g] >= TWO:
            @pl.loop(0, SIZES[g] // TWO)
            def _(n):
                second(STARTS[g] + TWO * n, TWO)
        if SIZES[g] % TWO:
            second(STARTS[g] + SIZES[g] - 1, 1)
        for rel in (1, QUART - 1, TWO):
            inner(g, rel).start()

    low = iota((M, L), 1) < N
    lane = iota((M, TWO * L), 1)

    def third(g):
        for rel in OTHERS:
            inner(g, rel).wait_recv()
        base = slot_of((y, c, 0))
        d = jnp.concatenate([dall[base], dall[base + 1]], axis=0)

        @pl.loop(0, SIZES[g] * QUART, unroll=QUART)
        def _(n):
            i = STARTS[g] + n // QUART
            jl = lax.rem(n, QUART)

            def column(s):
                row = pl.multiple_of((TWO * jl + s) * T, T)
                own = u2s[i, pl.ds(pl.multiple_of(mine * L + row, T), T), :]
                return jnp.concatenate([own] + [u2b[rel - 1, i, pl.ds(row, T), :] for rel in OTHERS], axis=0)

            out = dot(k3[...], jnp.concatenate([column(0), column(1)], axis=1))
            first, other = out[:M], out[M:]
            u3 = jnp.where(low, first[:, :L] + pltpu.roll(other[:, :L], N, 1),
                           pltpu.roll(first[:, L:], N, 1) + other[:, L:])
            at = i * T + S * z + TWO * jl
            even = jnp.sum(jnp.where(lane == at, d, 0.0), axis=1, keepdims=True)
            odd = jnp.sum(jnp.where(lane == at + 1, d, 0.0), axis=1, keepdims=True)
            w = jnp.where(low, even, odd) * u3.astype(BF16).astype(F32)
            wbuf[y * H + i, mine * QUART + jl] = w.astype(BF16)

    def share(g, kind, owner, dev):
        at = (pl.ds(owner[1] * H + STARTS[g], SIZES[g]), pl.ds(quarter(owner) * QUART, QUART))
        return send(wbuf.at[at], wbuf.at[at], ws_sem.at[g, kind], wr_sem.at[g, kind], dev)

    OWN_X, OWN_Y, OWN_P, X_Y, X_P, Y_P, D_P = range(KINDS)

    def gather_first(g):
        for kind, dev in ((OWN_X, in_x), (OWN_Y, in_y), (OWN_P, peer)):
            share(g, kind, (c, y, z), dev).start()
        if g == G:
            share(g, X_Y, (c, y, z), diagonal).start()

    def forward(g):
        share(g, OWN_X, in_x, in_x).wait_recv()
        if g != G:
            share(g, X_Y, in_x, in_y).start()
        share(g, X_P, in_x, peer).start()
        share(g, OWN_Y, in_y, in_y).wait_recv()
        share(g, Y_P, in_y, peer).start()

    def forward_diagonal(g):
        share(g, X_Y, diagonal, in_y).wait_recv()
        share(g, D_P, diagonal, peer).start()

    def gather_end(g):
        for kind, owner in ((OWN_P, (c, y, z)), (X_P, in_x), (Y_P, in_y), (D_P, diagonal)):
            share(g, kind, (oc,) + owner[1:], peer).wait_recv()

    low_v = iota((QUART, S, S, L), TWO + 1) < N

    def out_copy(p):
        slot = lax.rem(p, TWO)
        return pltpu.make_async_copy(
            v2s.at[slot], v2_out.at[:, :, pl.ds(pl.multiple_of(p * T, T), T), :], out_sem.at[slot])

    def middle(p):
        @pl.when(p >= TWO)
        def _():
            out_copy(p - TWO).wait()

        slot = lax.rem(p, TWO)
        for jo in range(TWO):
            rhs = jnp.concatenate(
                [wbuf[p + H * s, jo * S:(jo + 1) * S].reshape(TWO * L, L) for s in range(TWO)], axis=1)
            out = dot(l3[...], rhs)
            for s in range(TWO):
                o = out[:, s * L:(s + 1) * L].reshape(QUART, S, TWO, S, L)
                t0, t1 = o[:, :, 0], o[:, :, 1]
                even = jnp.where(low_v, t0, pltpu.roll(t1, N, TWO + 1))
                odd = jnp.where(low_v, pltpu.roll(t0, N, TWO + 1), t1)
                both = jnp.concatenate([even, odd], axis=TWO).astype(BF16)
                v3[:, s, jo * L:(jo + 1) * L, :] = both.reshape(QUART, L, L)
        for kb in range(QUART):
            out = dot(l2[...], jnp.concatenate([v3[kb, 0], v3[kb, 1]], axis=1))
            pair = jnp.concatenate([out[:, :L].reshape(N, S, L), out[:, L:].reshape(N, S, L)], axis=1)
            v2s[slot, kb] = pair.astype(BF16)
        out_copy(p).start()

    def all_middle(g, first=0, count=None):
        @pl.loop(STARTS[g] + first, STARTS[g] + (first + count if count else SIZES[g]))
        def _(p):
            middle(p)

    def arrived(g):
        for n in range(CHUNKS[g]):
            late(g, n).wait_recv()

    @pl.loop(0, STEPS)
    def _(t):
        early(t).wait_recv()

    for rel in DEVICES:
        diag(rel).wait_recv()
    all_second(A)
    all_second(B)
    third(A)
    gather_first(A)
    third(B)
    gather_first(B)
    depart(D)
    depart(E)
    arrived(C)
    all_second(C)
    forward(A)
    forward(B)
    third(C)
    gather_first(C)
    depart(G)
    forward_diagonal(A)
    gather_end(A)
    all_middle(A)
    forward_diagonal(B)
    arrived(D)
    all_second(D)
    gather_end(B)
    all_middle(B)
    third(D)
    gather_first(D)
    arrived(E)
    all_second(E)
    forward(C)
    third(E)
    gather_first(E)
    forward_diagonal(C)
    arrived(G)
    all_second(G)
    forward(D)
    gather_end(C)
    all_middle(C, 0, TWO)
    forward(E)
    third(G)
    gather_first(G)
    all_middle(C, TWO)
    forward_diagonal(D)
    gather_end(D)
    forward(G)
    all_middle(D)
    forward_diagonal(E)
    gather_end(E)
    all_middle(E)
    forward_diagonal(G)
    gather_end(G)
    all_middle(G)

    @pl.loop(0, STEPS)
    def _(t):
        early(t).wait_send()

    for rel in DEVICES:
        diag(rel).wait_send()
    for g in GROUPS:
        for n in range(CHUNKS[g]):
            late(g, n).wait_send()
        for rel in OTHERS:
            inner(g, rel).wait_send()
        for kind in range(KINDS):
            share(g, kind, (c, y, z), peer).wait_send()
    out_copy(H - TWO).wait()
    out_copy(H - 1).wait()


def compress(x, a1, a2, a3, b2_t, b3_t, d):
    vmem = pl.BlockSpec(memory_space=pltpu.VMEM)
    hbm = pl.BlockSpec(memory_space=pl.ANY)
    dma = pltpu.SemaphoreType.DMA
    u1 = pltpu.VMEM((N, H * T, L), BF16)
    spread = pltpu.VMEM((M * T, N * T), BF16)
    groups = len(SIZES)
    return pl.pallas_call(
        compress_body,
        out_shape=jax.ShapeDtypeStruct((QUART, N, M * S, L), BF16),
        in_specs=[hbm] + [vmem] * 6,
        out_specs=hbm,
        scratch_shapes=[
            pltpu.VMEM((NEAR, N, TWO, M, N), BF16), pltpu.VMEM((RING, N, TWO, M, N), BF16), u1, u1, u1,
            spread, spread, spread, spread, pltpu.VMEM((N, N), BF16),
            pltpu.VMEM((M * T, M * S), BF16), pltpu.VMEM((N * S, M * S), BF16),
            pltpu.VMEM((H, M * T, L), BF16), pltpu.VMEM((len(OTHERS), H, L, L), BF16),
            pltpu.VMEM((M, H, M, L), BF16), pltpu.VMEM((S, H, H * H), F32),
            pltpu.VMEM((QUART, TWO, M * S, L), BF16), pltpu.VMEM((TWO, QUART, N, T, L), BF16),
            dma((NEAR,)), dma((RING,)), dma((RING,)), pltpu.SemaphoreType.REGULAR,
            dma((STEPS,)), dma((STEPS,)), dma((groups, QUART)), dma((groups, QUART)),
            dma((groups, QUART)), dma((groups, QUART)), dma((groups, KINDS)), dma((groups, KINDS)),
            dma((KINDS,)), dma((KINDS,)), dma((TWO,)),
        ],
        compiler_params=pltpu.CompilerParams(collective_id=0, has_side_effects=True, vmem_limit_bytes=LIMIT),
        name="compress",
    )(x, a1, a2, a3, b2_t, b3_t, d)


def expand_body(v2_ref, b1_ref, z_ref, l1):
    @pl.when((pl.program_id(0) == 0) & (pl.program_id(1) == 0))
    def _():
        c = lax.axis_index("mx")
        fill(l1, b1_ref[...], lambda p: c * N + p // S, lambda q: lax.rem(q // S, TWO) * H + q // T, alike(S), dot_t)

    for j in range(0, z_ref.shape[1], TWO):
        out = dot(l1[...], jnp.concatenate([v2_ref[0, j], v2_ref[0, j + 1]], axis=1))
        for s in range(TWO):
            o = out[:, s * L:(s + 1) * L].reshape(N, S, L)
            z_ref[:, j + s, :S, :] = o[:, :, :N]
            z_ref[:, j + s, S:, :] = pltpu.roll(o, N, TWO)[:, :, :N]


def expand(v2, b1_t):
    return pl.pallas_call(
        expand_body,
        grid=(QUART, N // S),
        out_shape=jax.ShapeDtypeStruct((N, N, N, N), F32),
        in_specs=[pl.BlockSpec((1, S, M * S, L), lambda kb, jb: (kb, jb, 0, 0)),
                  pl.BlockSpec((M, L), lambda kb, jb: (0, 0))],
        out_specs=pl.BlockSpec((N, S, T, N), lambda kb, jb: (0, jb, kb, 0)),
        scratch_shapes=[pltpu.VMEM((N * S, M * S), BF16)],
        compiler_params=pltpu.CompilerParams(vmem_limit_bytes=LIMIT),
        name="expand",
    )(v2, b1_t)


def solution(mesh):
    vol_spec = P("mx", "my", "mz", "rhs")
    core_spec = P("mx", "my", "mz")
    full_spec = P()

    def local_operator(x_blk, fac_a1, fac_a2, fac_a3, diag_blk, fac_b1, fac_b2, fac_b3):
        v2 = compress(x_blk, fac_a1, fac_a2, fac_a3, fac_b2.T, fac_b3.T, diag_blk)
        return expand(v2, fac_b1.T)

    return jax.shard_map(local_operator, mesh=mesh, in_specs=(vol_spec, full_spec, full_spec, full_spec, core_spec, full_spec, full_spec, full_spec), out_specs=vol_spec, check_vma=False)
```

```python
import jax
import jax.numpy as jnp
from jax import lax
from jax.experimental import pallas as pl
from jax.experimental.pallas import tpu as pltpu
from jax.sharding import PartitionSpec as P

F32 = jnp.float32
BF16 = jnp.bfloat16
MESH = pl.DeviceIdType.MESH
N = 64
M = 32
L = 128
T = 16
S = 8
TWO = 2
QUART = 4
H = M // TWO
RING = 8
AHEAD = 4
NEAR = 4
STEPS = N // TWO
EARLY = 8
A, B, C, D, E, G = range(6)
SIZES = (4, 4, 4, 2, 1, 1)
STARTS = (0, 4, 8, 12, 14, 15)
CHUNKS = (0, 0, 4, 2, 1, 1)
FILLER = 8
GROUPS = range(len(SIZES))
OTHERS = range(1, QUART)
DEVICES = range(1, S)
KINDS = 7
COLUMNS = 16
LIMIT = 42 * 1024 * 1024


def dot(a, b):
    return jnp.dot(a, b, preferred_element_type=F32)


def dot_t(a, b):
    return lax.dot_general(a, b, (((0,), (0,)), ((), ())), preferred_element_type=F32)


def iota(shape, axis):
    return lax.broadcasted_iota(jnp.int32, shape, axis)


def ones_where(cond):
    return jnp.where(cond, 1.0, 0.0).astype(BF16)


def fill(out_ref, mat, row_of, col_of, keep, product=dot):
    rows, cols = out_ref.shape
    depth = mat.shape[1] if product is dot else mat.shape[0]
    wide = product(mat, ones_where(iota((depth, cols), 0) == col_of(iota((depth, cols), 1)))).astype(BF16)
    for r0 in range(0, rows, L):
        p = iota((L, wide.shape[0]), 0) + r0
        block = dot(ones_where(iota((L, wide.shape[0]), 1) == row_of(p)), wide)
        same = keep(iota((L, cols), 0) + r0, iota((L, cols), 1))
        out_ref[r0:r0 + L, :] = jnp.where(same, block, 0.0).astype(BF16)


def alike(n):
    return lambda p, q: lax.rem(p, n) == lax.rem(q, n)


def compress_body(x_hbm, a1_ref, a2_ref, a3_ref, b1_ref, b2_ref, b3_ref, d_ref, v2_out, l1_out,
                  xl, xr, u1o, u1s, u1r, k1o, k1r, k2o, k2r, k3, l3, l2, u2s, u2b, wbuf, dall, v3,
                  near_sem, xs_sem, xr_sem, credit, u1_sem, late_s, late_r,
                  u2_s, u2_r, w_s, w_r, d_sem):
    c = lax.axis_index("mx")
    y = lax.axis_index("my")
    z = lax.axis_index("mz")
    oc, oy, oz = 1 - c, 1 - y, 1 - z

    def flip(rel):
        return (lax.rem(c + rel // QUART, TWO), lax.rem(y + rel // TWO % TWO, TWO), lax.rem(z + rel % TWO, TWO))

    def beside(rel):
        return (lax.rem(c + rel // TWO, TWO), y, lax.rem(z + rel % TWO, TWO))

    def ids(dev):
        return dict(zip(("mx", "my", "mz"), dev))

    def send(src, dst, s_sem, r_sem, dev):
        return pltpu.make_async_remote_copy(src, dst, s_sem, r_sem, device_id=ids(dev), device_id_type=MESH)

    peer, in_x, in_y, diagonal = (oc, y, z), (c, oy, z), (c, y, oz), (c, oy, oz)

    barrier = pltpu.get_barrier_semaphore()
    for rel in DEVICES:
        pl.semaphore_signal(barrier, inc=1, device_id=ids(flip(rel)), device_id_type=MESH)

    def half_of(core, t):
        return x_hbm.at[:, pl.ds(TWO * t, TWO), pl.ds(core * M, M), :]

    def near(t):
        slot = lax.rem(t, NEAR)
        return pltpu.make_async_copy(half_of(c, t), xl.at[slot], near_sem.at[slot])

    def cross(t):
        slot = lax.rem(t, RING)
        return send(half_of(oc, t), xr.at[slot], xs_sem.at[slot], xr_sem.at[slot], peer)

    for t in range(NEAR - 1):
        near(t).start()

    def slot_of(dev):
        return QUART * dev[0] + TWO * dev[1] + dev[2]

    dall[slot_of((c, y, z))] = d_ref[...].reshape(H * H, H).T

    def rows_one(p):
        return lax.rem(p // T + H * y, M)

    fill(k1o, a1_ref[...], rows_one, lambda q: c * N + q // T, alike(T))
    fill(k1r, a1_ref[...], rows_one, lambda q: oc * N + q // T, alike(T))
    pl.semaphore_wait(barrier, len(DEVICES))
    for t in range(AHEAD):
        cross(t).start()

    my_slot = slot_of((c, y, z))

    def diag(rel):
        return send(dall.at[my_slot], dall.at[my_slot], d_sem.at[0], d_sem.at[1], flip(rel))

    for rel in DEVICES:
        diag(rel).start()

    def pack(ref, slot):
        parts = [jnp.concatenate([ref[slot, :, s, 0:T, :], ref[slot, :, s, T:M, :]], axis=-1).reshape(N * T, L)
                 for s in range(TWO)]
        return jnp.concatenate(parts, axis=1)

    def early(t):
        part = (pl.ds(TWO * t, TWO), pl.ds(0, EARLY * T))
        return send(u1s.at[part], u1r.at[part], u1_sem.at[0], u1_sem.at[1], in_x)

    def late(g, n):
        span = N // CHUNKS[g]
        part = (pl.ds(span * n, span), pl.ds(STARTS[g] * T, SIZES[g] * T))
        return send(u1s.at[part], u1r.at[part], late_s, late_r.at[g], in_x)

    @pl.loop(0, STEPS)
    def _(t):
        @pl.when(t + NEAR - 1 < STEPS)
        def _():
            near(t + NEAR - 1).start()

        @pl.when(t >= 1)
        def _():
            early(t - 1).start()

        @pl.when(t == 2 * FILLER + 1)
        def _():
            late(C, 0).start()

        near(t).wait()
        cross(t).wait_recv()
        acc = dot(k1o[...], pack(xl, lax.rem(t, NEAR))) + dot(k1r[...], pack(xr, lax.rem(t, RING)))
        u1 = acc.astype(BF16)
        for s in range(TWO):
            u1o[TWO * t + s] = u1[:H * T, s * L:(s + 1) * L]
            u1s[TWO * t + s] = u1[H * T:, s * L:(s + 1) * L]

        @pl.when(t < STEPS - RING)
        def _():
            pl.semaphore_signal(credit, inc=1, device_id=ids(peer), device_id_type=MESH)

        @pl.when(t + AHEAD >= RING)
        def _():
            cross(t + AHEAD - RING).wait_send()

        @pl.when((t + AHEAD >= RING) & (t + AHEAD < STEPS))
        def _():
            pl.semaphore_wait(credit, 1)

        @pl.when(t + AHEAD < STEPS)
        def _():
            cross(t + AHEAD).start()

    def depart(g, first=0):
        for n in range(first, CHUNKS[g]):
            late(g, n).start()

    early(STEPS - 1).start()
    depart(C, 1)
    for t in range(STEPS - RING + AHEAD, STEPS):
        cross(t).wait_send()

    fill(k2o, a2_ref[...], lambda p: p // T, lambda q: y * N + q // T, alike(T))
    fill(k2r, a2_ref[...], lambda p: p // T, lambda q: oy * N + q // T, alike(T))
    q = iota((L, N), 1)
    k_first = lax.rem(z + q // T % TWO, TWO) * N + lax.rem(c + q // M, TWO) * M + lax.rem(q, T)
    for half in range(TWO):
        sel = ones_where(iota((L, N), 0) == k_first + T * half)
        k3[half * M:(half + 1) * M, :] = dot(a3_ref[...], sel).astype(BF16)
    fill(l2, b2_ref[...], lambda p: y * N + p // S, lambda q: q // S, alike(S), dot_t)
    fill(l1_out, b1_ref[...], lambda p: c * N + p // S, lambda q: lax.rem(q // S, TWO) * H + q // T, alike(S), dot_t)
    fill(l3, b3_ref[...], lambda p: z * N + p // L * T + lax.rem(p, T), lambda q: lax.rem(q, M),
         lambda p, q: lax.rem(p, L) // T == q // M, dot_t)

    def second(i, width):
        def side(ref):
            return jnp.concatenate(
                [ref[:, pl.ds(pl.multiple_of((i + s) * T, T), T), :].reshape(N * T, L) for s in range(width)], axis=1)

        out = dot(k2o[...], side(u1o)) + dot(k2r[...], side(u1r))
        for s in range(width):
            u2s[i + s] = out[:, s * L:(s + 1) * L].astype(BF16)

    def quarter(dev):
        return TWO * dev[0] + dev[2]

    mine = quarter((c, y, z))

    def inner(g, rel):
        dev = beside(rel)
        i_span = pl.ds(STARTS[g], SIZES[g])
        return send(u2s.at[i_span, pl.ds(quarter(dev) * L, L)], u2b.at[rel - 1, i_span],
                    u2_s, u2_r.at[g], dev)

    def all_second(g):
        if SIZES[g] >= TWO:
            @pl.loop(0, SIZES[g] // TWO)
            def _(n):
                second(STARTS[g] + TWO * n, TWO)
        if SIZES[g] % TWO:
            second(STARTS[g] + SIZES[g] - 1, 1)
        for rel in (1, QUART - 1, TWO):
            inner(g, rel).start()

    low = iota((M, L), 1) < N
    lane = iota((M, TWO * L), 1)

    def third(g):
        got = u2b.at[:, pl.ds(STARTS[g], SIZES[g])]
        send(got, got, u2_s, u2_r.at[g], peer).wait_recv()
        base = slot_of((y, c, 0))
        d = jnp.concatenate([dall[base], dall[base + 1]], axis=0)

        @pl.loop(0, SIZES[g] * QUART, unroll=QUART)
        def _(n):
            i = STARTS[g] + n // QUART
            jl = lax.rem(n, QUART)

            def column(s):
                row = pl.multiple_of((TWO * jl + s) * T, T)
                own = u2s[i, pl.ds(pl.multiple_of(mine * L + row, T), T), :]
                return jnp.concatenate([own] + [u2b[rel - 1, i, pl.ds(row, T), :] for rel in OTHERS], axis=0)

            out = dot(k3[...], jnp.concatenate([column(0), column(1)], axis=1))
            first, other = out[:M], out[M:]
            u3 = jnp.where(low, first[:, :L] + pltpu.roll(other[:, :L], N, 1),
                           pltpu.roll(first[:, L:], N, 1) + other[:, L:])
            at = i * T + S * z + TWO * jl
            even = jnp.sum(jnp.where(lane == at, d, 0.0), axis=1, keepdims=True)
            odd = jnp.sum(jnp.where(lane == at + 1, d, 0.0), axis=1, keepdims=True)
            w = jnp.where(low, even, odd) * u3.astype(BF16).astype(F32)
            wbuf[y * H + i, mine * QUART + jl] = w.astype(BF16)

    def share(g, kind, owner, dev):
        at = (pl.ds(owner[1] * H + STARTS[g], SIZES[g]), pl.ds(quarter(owner) * QUART, QUART))
        return send(wbuf.at[at], wbuf.at[at], w_s, w_r.at[g, min(kind, FROM_P)], dev)

    OWN_X, OWN_Y, X_Y, OWN_P, X_P, Y_P, D_P = range(KINDS)
    FROM_P = OWN_P

    def gather_first(g):
        for kind, dev in ((OWN_X, in_x), (OWN_Y, in_y), (OWN_P, peer)):
            share(g, kind, (c, y, z), dev).start()
        if g == G:
            share(g, X_Y, (c, y, z), diagonal).start()

    def forward(g):
        share(g, OWN_X, in_x, in_x).wait_recv()
        if g != G:
            share(g, X_Y, in_x, in_y).start()
        share(g, X_P, in_x, peer).start()
        share(g, OWN_Y, in_y, in_y).wait_recv()
        share(g, Y_P, in_y, peer).start()

    def forward_diagonal(g):
        share(g, X_Y, diagonal, in_y).wait_recv()
        share(g, D_P, diagonal, peer).start()

    def gather_end(g):
        got = wbuf.at[pl.ds(0, SIZES[g]), :]
        send(got, got, w_s, w_r.at[g, FROM_P], peer).wait_recv()

    low_v = iota((QUART, S, S, L), TWO + 1) < N

    def middle(p):
        for jo in range(TWO):
            rhs = jnp.concatenate(
                [wbuf[p + H * s, jo * S:(jo + 1) * S].reshape(TWO * L, L) for s in range(TWO)], axis=1)
            out = dot(l3[...], rhs)
            for s in range(TWO):
                o = out[:, s * L:(s + 1) * L].reshape(QUART, S, TWO, S, L)
                t0, t1 = o[:, :, 0], o[:, :, 1]
                even = jnp.where(low_v, t0, pltpu.roll(t1, N, TWO + 1))
                odd = jnp.where(low_v, pltpu.roll(t0, N, TWO + 1), t1)
                both = jnp.concatenate([even, odd], axis=TWO).astype(BF16)
                v3[:, s, jo * L:(jo + 1) * L, :] = both.reshape(QUART, L, L)
        for kb in range(QUART):
            out = dot(l2[...], jnp.concatenate([v3[kb, 0], v3[kb, 1]], axis=1))
            pair = jnp.concatenate([out[:, :L].reshape(N, S, L), out[:, L:].reshape(N, S, L)], axis=1)
            v2_out[kb, :, pl.ds(pl.multiple_of(p * T, T), T), :] = pair.astype(BF16)

    def all_middle(g):
        @pl.loop(STARTS[g], STARTS[g] + SIZES[g])
        def _(p):
            middle(p)

    def arrived(g):
        got = u1r.at[:, pl.ds(STARTS[g] * T, SIZES[g] * T)]
        send(got, got, late_s, late_r.at[g], in_x).wait_recv()

    first = u1r.at[:, pl.ds(0, EARLY * T)]
    rest = u1r.at[:, pl.ds(EARLY * T, EARLY * T)]
    cores = dall.at[pl.ds(0, len(DEVICES))]
    send(first, first, u1_sem.at[0], u1_sem.at[1], in_x).wait_recv()
    send(cores, cores, d_sem.at[0], d_sem.at[1], peer).wait_recv()
    all_second(A)
    all_second(B)
    third(A)
    gather_first(A)
    third(B)
    gather_first(B)
    depart(D)
    arrived(C)
    all_second(C)
    forward(A)
    forward(B)
    third(C)
    gather_first(C)
    depart(E)
    depart(G)
    forward_diagonal(A)
    gather_end(A)
    all_middle(A)
    forward_diagonal(B)
    arrived(D)
    all_second(D)
    forward(C)
    gather_end(B)
    all_middle(B)
    third(D)
    gather_first(D)
    forward_diagonal(C)
    arrived(E)
    all_second(E)
    gather_end(C)
    all_middle(C)
    third(E)
    gather_first(E)
    arrived(G)
    all_second(G)
    forward(D)
    forward(E)
    third(G)
    gather_first(G)
    forward_diagonal(D)
    gather_end(D)
    all_middle(D)
    forward_diagonal(E)
    gather_end(E)
    forward(G)
    all_middle(E)
    forward_diagonal(G)
    gather_end(G)
    all_middle(G)

    sent = wbuf.at[pl.ds(0, KINDS * QUART), :]
    send(first, first, u1_sem.at[0], u1_sem.at[1], in_x).wait_send()
    send(rest, rest, late_s, late_r.at[0], in_x).wait_send()
    send(cores, cores, d_sem.at[0], d_sem.at[1], peer).wait_send()
    send(u2b, u2b, u2_s, u2_r.at[0], peer).wait_send()
    send(sent, sent, w_s, w_r.at[0, 0], peer).wait_send()


def compress(x, a1, a2, a3, b1_t, b2_t, b3_t, d):
    vmem = pl.BlockSpec(memory_space=pltpu.VMEM)
    hbm = pl.BlockSpec(memory_space=pl.ANY)
    dma = pltpu.SemaphoreType.DMA
    u1 = pltpu.VMEM((N, H * T, L), BF16)
    spread = pltpu.VMEM((M * T, N * T), BF16)
    groups = len(SIZES)
    return pl.pallas_call(
        compress_body,
        out_shape=(pltpu.VMEM((QUART, N, M * S, L), BF16), pltpu.VMEM((N * S, M * S), BF16)),
        in_specs=[hbm] + [vmem] * 7,
        out_specs=(vmem, vmem),
        scratch_shapes=[
            pltpu.VMEM((NEAR, N, TWO, M, N), BF16), pltpu.VMEM((RING, N, TWO, M, N), BF16), u1, u1, u1,
            spread, spread, spread, spread, pltpu.VMEM((N, N), BF16),
            pltpu.VMEM((M * T, M * S), BF16), pltpu.VMEM((N * S, M * S), BF16),
            pltpu.VMEM((H, M * T, L), BF16), pltpu.VMEM((len(OTHERS), H, L, L), BF16),
            pltpu.VMEM((M, H, M, L), BF16), pltpu.VMEM((S, H, H * H), F32),
            pltpu.VMEM((QUART, TWO, M * S, L), BF16),
            dma((NEAR,)), dma((RING,)), dma((RING,)), pltpu.SemaphoreType.REGULAR,
            dma((TWO,)), dma, dma((groups,)), dma, dma((groups,)), dma, dma((groups, QUART)), dma((TWO,)),
        ],
        compiler_params=pltpu.CompilerParams(collective_id=0, has_side_effects=True, vmem_limit_bytes=LIMIT),
        name="compress",
    )(x, a1, a2, a3, b1_t, b2_t, b3_t, d)


def expand_body(v2_ref, l1_ref, z_ref):
    for j in range(0, COLUMNS, TWO):
        out = dot(l1_ref[...], jnp.concatenate([v2_ref[0, j], v2_ref[0, j + 1]], axis=1))
        for s in range(TWO):
            o = out[:, s * L:(s + 1) * L].reshape(N, S, L)
            z_ref[:, j + s, :S, :] = o[:, :, :N]
            z_ref[:, j + s, S:, :] = pltpu.roll(o, N, TWO)[:, :, :N]


def expand(v2, l1):
    return pl.pallas_call(
        expand_body,
        grid=(QUART, N // COLUMNS),
        out_shape=jax.ShapeDtypeStruct((N, N, N, N), F32),
        in_specs=[pl.BlockSpec((1, COLUMNS, M * S, L), lambda kb, jb: (kb, jb, 0, 0)),
                  pl.BlockSpec((N * S, M * S), lambda kb, jb: (0, 0))],
        out_specs=pl.BlockSpec((N, COLUMNS, T, N), lambda kb, jb: (0, jb, kb, 0)),
        compiler_params=pltpu.CompilerParams(vmem_limit_bytes=LIMIT // 2),
        name="expand",
    )(v2, l1)


def solution(mesh):
    vol_spec = P("mx", "my", "mz", "rhs")
    core_spec = P("mx", "my", "mz")
    full_spec = P()

    def local_operator(x_blk, fac_a1, fac_a2, fac_a3, diag_blk, fac_b1, fac_b2, fac_b3):
        v2, l1 = compress(x_blk, fac_a1, fac_a2, fac_a3, fac_b1.T, fac_b2.T, fac_b3.T, diag_blk)
        return expand(v2, l1)

    return jax.shard_map(local_operator, mesh=mesh, in_specs=(vol_spec, full_spec, full_spec, full_spec, core_spec, full_spec, full_spec, full_spec), out_specs=vol_spec, check_vma=False)
```

```python
import jax
import jax.numpy as jnp
from jax import lax
from jax.experimental import pallas as pl
from jax.experimental.pallas import tpu as pltpu
from jax.sharding import PartitionSpec as P

F32 = jnp.float32
BF16 = jnp.bfloat16
MESH = pl.DeviceIdType.MESH
N = 64
M = 32
L = 128
T = 16
S = 8
TWO = 2
QUART = 4
H = M // TWO
RING = 8
AHEAD = 4
NEAR = 4
STEPS = N // TWO
EARLY = 8
A, B, C, D, E, G = range(6)
SIZES = (4, 4, 4, 2, 1, 1)
STARTS = (0, 4, 8, 12, 14, 15)
CHUNKS = (0, 0, 4, 2, 1, 1)
FILLER = 8
GROUPS = range(len(SIZES))
OTHERS = range(1, QUART)
DEVICES = range(1, S)
KINDS = 7
COLUMNS = 4
SLOTS = 4
LIMIT = 42 * 1024 * 1024


def dot(a, b):
    return jnp.dot(a, b, preferred_element_type=F32)


def dot_t(a, b):
    return lax.dot_general(a, b, (((0,), (0,)), ((), ())), preferred_element_type=F32)


def iota(shape, axis):
    return lax.broadcasted_iota(jnp.int32, shape, axis)


def ones_where(cond):
    return jnp.where(cond, 1.0, 0.0).astype(BF16)


def fill(out_ref, mat, row_of, col_of, keep, product=dot):
    rows, cols = out_ref.shape
    depth = mat.shape[1] if product is dot else mat.shape[0]
    wide = product(mat, ones_where(iota((depth, cols), 0) == col_of(iota((depth, cols), 1)))).astype(BF16)
    for r0 in range(0, rows, L):
        p = iota((L, wide.shape[0]), 0) + r0
        block = dot(ones_where(iota((L, wide.shape[0]), 1) == row_of(p)), wide)
        same = keep(iota((L, cols), 0) + r0, iota((L, cols), 1))
        out_ref[r0:r0 + L, :] = jnp.where(same, block, 0.0).astype(BF16)


def alike(n):
    return lambda p, q: lax.rem(p, n) == lax.rem(q, n)


def compress_body(x_hbm, a1_ref, a2_ref, a3_ref, b1_ref, b2_ref, b3_ref, d_ref, v2_out, l1_out,
                  xl, xr, u1o, u1s, u1r, k1o, k1r, k2o, k2r, k3, l3, l2, u2s, u2b, wbuf, dall, v3,
                  near_sem, xs_sem, xr_sem, credit, u1_sem, late_s, late_r,
                  u2_s, u2_r, w_s, w_r, d_sem):
    c = lax.axis_index("mx")
    y = lax.axis_index("my")
    z = lax.axis_index("mz")
    oc, oy, oz = 1 - c, 1 - y, 1 - z

    def flip(rel):
        return (lax.rem(c + rel // QUART, TWO), lax.rem(y + rel // TWO % TWO, TWO), lax.rem(z + rel % TWO, TWO))

    def beside(rel):
        return (lax.rem(c + rel // TWO, TWO), y, lax.rem(z + rel % TWO, TWO))

    def ids(dev):
        return dict(zip(("mx", "my", "mz"), dev))

    def send(src, dst, s_sem, r_sem, dev):
        return pltpu.make_async_remote_copy(src, dst, s_sem, r_sem, device_id=ids(dev), device_id_type=MESH)

    peer, in_x, in_y, diagonal = (oc, y, z), (c, oy, z), (c, y, oz), (c, oy, oz)

    barrier = pltpu.get_barrier_semaphore()
    for rel in DEVICES:
        pl.semaphore_signal(barrier, inc=1, device_id=ids(flip(rel)), device_id_type=MESH)

    def half_of(core, t):
        return x_hbm.at[:, pl.ds(TWO * t, TWO), pl.ds(core * M, M), :]

    def near(t):
        slot = lax.rem(t, NEAR)
        return pltpu.make_async_copy(half_of(c, t), xl.at[slot], near_sem.at[slot])

    def cross(t):
        slot = lax.rem(t, RING)
        return send(half_of(oc, t), xr.at[slot], xs_sem.at[slot], xr_sem.at[slot], peer)

    pl.semaphore_wait(barrier, len(DEVICES))
    for t in range(AHEAD):
        cross(t).start()
    for t in range(NEAR - 1):
        near(t).start()

    def slot_of(dev):
        return QUART * dev[0] + TWO * dev[1] + dev[2]

    dall[slot_of((c, y, z))] = d_ref[...].reshape(H * H, H).T

    def rows_one(p):
        return lax.rem(p // T + H * y, M)

    fill(k1o, a1_ref[...], rows_one, lambda q: c * N + q // T, alike(T))
    fill(k1r, a1_ref[...], rows_one, lambda q: oc * N + q // T, alike(T))

    my_slot = slot_of((c, y, z))

    def diag(rel):
        return send(dall.at[my_slot], dall.at[my_slot], d_sem.at[0], d_sem.at[1], flip(rel))

    for rel in DEVICES:
        diag(rel).start()

    def pack(ref, slot):
        parts = [jnp.concatenate([ref[slot, :, s, 0:T, :], ref[slot, :, s, T:M, :]], axis=-1).reshape(N * T, L)
                 for s in range(TWO)]
        return jnp.concatenate(parts, axis=1)

    def early(t):
        part = (pl.ds(TWO * t, TWO), pl.ds(0, EARLY * T))
        return send(u1s.at[part], u1r.at[part], u1_sem.at[0], u1_sem.at[1], in_x)

    def late(g, n):
        span = N // CHUNKS[g]
        part = (pl.ds(span * n, span), pl.ds(STARTS[g] * T, SIZES[g] * T))
        return send(u1s.at[part], u1r.at[part], late_s, late_r.at[g], in_x)

    @pl.loop(0, STEPS)
    def _(t):
        @pl.when(t + NEAR - 1 < STEPS)
        def _():
            near(t + NEAR - 1).start()

        @pl.when(t >= 1)
        def _():
            early(t - 1).start()

        @pl.when(t == FILLER + 1)
        def _():
            late(C, 0).start()

        near(t).wait()
        cross(t).wait_recv()
        acc = dot(k1o[...], pack(xl, lax.rem(t, NEAR))) + dot(k1r[...], pack(xr, lax.rem(t, RING)))
        u1 = acc.astype(BF16)
        for s in range(TWO):
            u1o[TWO * t + s] = u1[:H * T, s * L:(s + 1) * L]
            u1s[TWO * t + s] = u1[H * T:, s * L:(s + 1) * L]

        @pl.when(t < STEPS - RING)
        def _():
            pl.semaphore_signal(credit, inc=1, device_id=ids(peer), device_id_type=MESH)

        @pl.when(t + AHEAD >= RING)
        def _():
            cross(t + AHEAD - RING).wait_send()

        @pl.when((t + AHEAD >= RING) & (t + AHEAD < STEPS))
        def _():
            pl.semaphore_wait(credit, 1)

        @pl.when(t + AHEAD < STEPS)
        def _():
            cross(t + AHEAD).start()

    def depart(g, first=0):
        for n in range(first, CHUNKS[g]):
            late(g, n).start()

    early(STEPS - 1).start()
    depart(C, 1)
    for t in range(STEPS - RING + AHEAD, STEPS):
        cross(t).wait_send()

    fill(k2o, a2_ref[...], lambda p: p // T, lambda q: y * N + q // T, alike(T))
    fill(k2r, a2_ref[...], lambda p: p // T, lambda q: oy * N + q // T, alike(T))
    q = iota((L, N), 1)
    k_first = lax.rem(z + q // T % TWO, TWO) * N + lax.rem(c + q // M, TWO) * M + lax.rem(q, T)
    for half in range(TWO):
        sel = ones_where(iota((L, N), 0) == k_first + T * half)
        k3[half * M:(half + 1) * M, :] = dot(a3_ref[...], sel).astype(BF16)
    fill(l2, b2_ref[...], lambda p: y * N + p // S, lambda q: q // S, alike(S), dot_t)
    fill(l1_out, b1_ref[...], lambda p: c * N + p // S, lambda q: lax.rem(q // S, TWO) * H + q // T, alike(S), dot_t)
    fill(l3, b3_ref[...], lambda p: z * N + p // L * T + lax.rem(p, T), lambda q: lax.rem(q, M),
         lambda p, q: lax.rem(p, L) // T == q // M, dot_t)

    def second(i, width):
        def side(ref):
            return jnp.concatenate(
                [ref[:, pl.ds(pl.multiple_of((i + s) * T, T), T), :].reshape(N * T, L) for s in range(width)], axis=1)

        out = dot(k2o[...], side(u1o)) + dot(k2r[...], side(u1r))
        for s in range(width):
            u2s[i + s] = out[:, s * L:(s + 1) * L].astype(BF16)

    def quarter(dev):
        return TWO * dev[0] + dev[2]

    mine = quarter((c, y, z))

    def inner(g, rel):
        dev = beside(rel)
        i_span = pl.ds(STARTS[g], SIZES[g])
        return send(u2s.at[i_span, pl.ds(quarter(dev) * L, L)], u2b.at[rel - 1, i_span],
                    u2_s, u2_r.at[g], dev)

    def all_second(g):
        if SIZES[g] >= TWO:
            @pl.loop(0, SIZES[g] // TWO)
            def _(n):
                second(STARTS[g] + TWO * n, TWO)
        if SIZES[g] % TWO:
            second(STARTS[g] + SIZES[g] - 1, 1)
        for rel in (1, QUART - 1, TWO):
            inner(g, rel).start()

    low = iota((M, L), 1) < N
    lane = iota((M, TWO * L), 1)

    def third(g):
        got = u2b.at[:, pl.ds(STARTS[g], SIZES[g])]
        send(got, got, u2_s, u2_r.at[g], peer).wait_recv()
        base = slot_of((y, c, 0))
        d = jnp.concatenate([dall[base], dall[base + 1]], axis=0)

        @pl.loop(0, SIZES[g] * QUART, unroll=QUART)
        def _(n):
            i = STARTS[g] + n // QUART
            jl = lax.rem(n, QUART)

            def column(s):
                row = pl.multiple_of((TWO * jl + s) * T, T)
                own = u2s[i, pl.ds(pl.multiple_of(mine * L + row, T), T), :]
                return jnp.concatenate([own] + [u2b[rel - 1, i, pl.ds(row, T), :] for rel in OTHERS], axis=0)

            out = dot(k3[...], jnp.concatenate([column(0), column(1)], axis=1))
            first, other = out[:M], out[M:]
            u3 = jnp.where(low, first[:, :L] + pltpu.roll(other[:, :L], N, 1),
                           pltpu.roll(first[:, L:], N, 1) + other[:, L:])
            at = i * T + S * z + TWO * jl
            even = jnp.sum(jnp.where(lane == at, d, 0.0), axis=1, keepdims=True)
            odd = jnp.sum(jnp.where(lane == at + 1, d, 0.0), axis=1, keepdims=True)
            w = jnp.where(low, even, odd) * u3.astype(BF16).astype(F32)
            wbuf[y * H + i, mine * QUART + jl] = w.astype(BF16)

    def share(g, kind, owner, dev):
        at = (pl.ds(owner[1] * H + STARTS[g], SIZES[g]), pl.ds(quarter(owner) * QUART, QUART))
        return send(wbuf.at[at], wbuf.at[at], w_s, w_r.at[g, min(kind, FROM_P)], dev)

    OWN_X, OWN_Y, X_Y, OWN_P, X_P, Y_P, D_P = range(KINDS)
    FROM_P = OWN_P

    def gather_first(g):
        for kind, dev in ((OWN_X, in_x), (OWN_Y, in_y), (OWN_P, peer)):
            share(g, kind, (c, y, z), dev).start()
        if g == G:
            share(g, X_Y, (c, y, z), diagonal).start()

    def forward(g):
        share(g, OWN_X, in_x, in_x).wait_recv()
        if g != G:
            share(g, X_Y, in_x, in_y).start()
        share(g, X_P, in_x, peer).start()
        share(g, OWN_Y, in_y, in_y).wait_recv()
        share(g, Y_P, in_y, peer).start()

    def forward_diagonal(g):
        share(g, X_Y, diagonal, in_y).wait_recv()
        share(g, D_P, diagonal, peer).start()

    def gather_end(g):
        got = wbuf.at[pl.ds(0, SIZES[g]), :]
        send(got, got, w_s, w_r.at[g, FROM_P], peer).wait_recv()

    low_v = iota((QUART, S, S, L), TWO + 1) < N

    def middle(p):
        for jo in range(TWO):
            rhs = jnp.concatenate(
                [wbuf[p + H * s, jo * S:(jo + 1) * S].reshape(TWO * L, L) for s in range(TWO)], axis=1)
            out = dot(l3[...], rhs)
            for s in range(TWO):
                o = out[:, s * L:(s + 1) * L].reshape(QUART, S, TWO, S, L)
                t0, t1 = o[:, :, 0], o[:, :, 1]
                even = jnp.where(low_v, t0, pltpu.roll(t1, N, TWO + 1))
                odd = jnp.where(low_v, pltpu.roll(t0, N, TWO + 1), t1)
                both = jnp.concatenate([even, odd], axis=TWO).astype(BF16)
                v3[:, s, jo * L:(jo + 1) * L, :] = both.reshape(QUART, L, L)
        for kb in range(QUART):
            out = dot(l2[...], jnp.concatenate([v3[kb, 0], v3[kb, 1]], axis=1))
            pair = jnp.concatenate([out[:, :L].reshape(N, S, L), out[:, L:].reshape(N, S, L)], axis=1)
            v2_out[kb, :, pl.ds(pl.multiple_of(p * T, T), T), :] = pair.astype(BF16)

    def all_middle(g):
        @pl.loop(STARTS[g], STARTS[g] + SIZES[g])
        def _(p):
            middle(p)

    def arrived(g):
        got = u1r.at[:, pl.ds(STARTS[g] * T, SIZES[g] * T)]
        send(got, got, late_s, late_r.at[g], in_x).wait_recv()

    first = u1r.at[:, pl.ds(0, EARLY * T)]
    rest = u1r.at[:, pl.ds(EARLY * T, EARLY * T)]
    cores = dall.at[pl.ds(0, len(DEVICES))]
    send(first, first, u1_sem.at[0], u1_sem.at[1], in_x).wait_recv()
    send(cores, cores, d_sem.at[0], d_sem.at[1], peer).wait_recv()
    all_second(A)
    all_second(B)
    third(A)
    gather_first(A)
    third(B)
    gather_first(B)
    depart(D)
    arrived(C)
    all_second(C)
    forward(A)
    forward(B)
    third(C)
    gather_first(C)
    depart(E)
    depart(G)
    forward_diagonal(A)
    gather_end(A)
    all_middle(A)
    forward_diagonal(B)
    arrived(D)
    all_second(D)
    forward(C)
    gather_end(B)
    all_middle(B)
    third(D)
    gather_first(D)
    forward_diagonal(C)
    arrived(E)
    all_second(E)
    gather_end(C)
    all_middle(C)
    third(E)
    gather_first(E)
    arrived(G)
    all_second(G)
    forward(D)
    forward(E)
    third(G)
    gather_first(G)
    forward_diagonal(D)
    forward_diagonal(E)
    gather_end(D)
    all_middle(D)
    forward(G)
    forward_diagonal(G)
    gather_end(E)
    all_middle(E)
    gather_end(G)
    all_middle(G)

    sent = wbuf.at[pl.ds(0, KINDS * QUART), :]
    send(first, first, u1_sem.at[0], u1_sem.at[1], in_x).wait_send()
    send(rest, rest, late_s, late_r.at[0], in_x).wait_send()
    send(cores, cores, d_sem.at[0], d_sem.at[1], peer).wait_send()
    send(u2b, u2b, u2_s, u2_r.at[0], peer).wait_send()
    send(sent, sent, w_s, w_r.at[0, 0], peer).wait_send()


def compress(x, a1, a2, a3, b1_t, b2_t, b3_t, d):
    vmem = pl.BlockSpec(memory_space=pltpu.VMEM)
    hbm = pl.BlockSpec(memory_space=pl.ANY)
    dma = pltpu.SemaphoreType.DMA
    u1 = pltpu.VMEM((N, H * T, L), BF16)
    spread = pltpu.VMEM((M * T, N * T), BF16)
    groups = len(SIZES)
    return pl.pallas_call(
        compress_body,
        out_shape=(pltpu.VMEM((QUART, N, M * S, L), BF16), pltpu.VMEM((N * S, M * S), BF16)),
        in_specs=[hbm] + [vmem] * 7,
        out_specs=(vmem, vmem),
        scratch_shapes=[
            pltpu.VMEM((NEAR, N, TWO, M, N), BF16), pltpu.VMEM((RING, N, TWO, M, N), BF16), u1, u1, u1,
            spread, spread, spread, spread, pltpu.VMEM((N, N), BF16),
            pltpu.VMEM((M * T, M * S), BF16), pltpu.VMEM((N * S, M * S), BF16),
            pltpu.VMEM((H, M * T, L), BF16), pltpu.VMEM((len(OTHERS), H, L, L), BF16),
            pltpu.VMEM((M, H, M, L), BF16), pltpu.VMEM((S, H, H * H), F32),
            pltpu.VMEM((QUART, TWO, M * S, L), BF16),
            dma((NEAR,)), dma((RING,)), dma((RING,)), pltpu.SemaphoreType.REGULAR,
            dma((TWO,)), dma, dma((groups,)), dma, dma((groups,)), dma, dma((groups, QUART)), dma((TWO,)),
        ],
        compiler_params=pltpu.CompilerParams(collective_id=0, has_side_effects=True, vmem_limit_bytes=LIMIT),
        name="compress",
    )(x, a1, a2, a3, b1_t, b2_t, b3_t, d)


def expand_body(v2_ref, l1_ref, z_hbm, zbuf, z_sem):
    per_block = N // COLUMNS

    def leave(n):
        slot = lax.rem(n, SLOTS)
        where = (slice(None), pl.ds(n % per_block * COLUMNS, COLUMNS), pl.ds(n // per_block * T, T))
        return pltpu.make_async_copy(zbuf.at[slot], z_hbm.at[where], z_sem.at[slot])

    @pl.loop(0, QUART * per_block)
    def _(n):
        slot = lax.rem(n, SLOTS)

        @pl.when(n >= SLOTS)
        def _():
            leave(n - SLOTS).wait()

        for j in range(0, COLUMNS, TWO):
            at = n % per_block * COLUMNS + j
            out = dot(l1_ref[...], jnp.concatenate([v2_ref[n // per_block, at + s] for s in range(TWO)], axis=1))
            for s in range(TWO):
                o = out[:, s * L:(s + 1) * L].reshape(N, S, L)
                zbuf[slot, :, j + s, :S, :] = o[:, :, :N]
                zbuf[slot, :, j + s, S:, :] = pltpu.roll(o, N, TWO)[:, :, :N]
        leave(n).start()

    for n in range(QUART * per_block - SLOTS, QUART * per_block):
        leave(n).wait()


def expand(v2, l1):
    vmem = pl.BlockSpec(memory_space=pltpu.VMEM)
    return pl.pallas_call(
        expand_body,
        out_shape=jax.ShapeDtypeStruct((N, N, N, N), F32),
        in_specs=[vmem, vmem],
        out_specs=pl.BlockSpec(memory_space=pl.ANY),
        scratch_shapes=[pltpu.VMEM((SLOTS, N, COLUMNS, T, N), F32), pltpu.SemaphoreType.DMA((SLOTS,))],
        compiler_params=pltpu.CompilerParams(vmem_limit_bytes=LIMIT // 2),
        name="expand",
    )(v2, l1)


def solution(mesh):
    vol_spec = P("mx", "my", "mz", "rhs")
    core_spec = P("mx", "my", "mz")
    full_spec = P()

    def local_operator(x_blk, fac_a1, fac_a2, fac_a3, diag_blk, fac_b1, fac_b2, fac_b3):
        v2, l1 = compress(x_blk, fac_a1, fac_a2, fac_a3, fac_b1.T, fac_b2.T, fac_b3.T, diag_blk)
        return expand(v2, l1)

    return jax.shard_map(local_operator, mesh=mesh, in_specs=(vol_spec, full_spec, full_spec, full_spec, core_spec, full_spec, full_spec, full_spec), out_specs=vol_spec, check_vma=False)
```

```python
import jax
import jax.numpy as jnp
from jax import lax
from jax.experimental import pallas as pl
from jax.experimental.pallas import tpu as pltpu
from jax.sharding import PartitionSpec as P

F32 = jnp.float32
BF16 = jnp.bfloat16
MESH = pl.DeviceIdType.MESH
N = 64
M = 32
L = 128
T = 16
S = 8
TWO = 2
QUART = 4
H = M // TWO
RING = 8
AHEAD = 4
NEAR = 4
STEPS = N // TWO
EARLY = 8
A, B, C, D, E, F, G = range(7)
SIZES = (4, 4, 2, 2, 2, 1, 1)
STARTS = (0, 4, 8, 10, 12, 14, 15)
CHUNKS = (0, 0, 4, 2, 2, 1, 1)
DIRECT = (F, G)
FILLERS = 2
GROUPS = range(len(SIZES))
OTHERS = range(1, QUART)
DEVICES = range(1, S)
KINDS = 7
COLUMNS = 4
SLOTS = 4
LIMIT = 42 * 1024 * 1024


def dot(a, b):
    return jnp.dot(a, b, preferred_element_type=F32)


def dot_t(a, b):
    return lax.dot_general(a, b, (((0,), (0,)), ((), ())), preferred_element_type=F32)


def iota(shape, axis):
    return lax.broadcasted_iota(jnp.int32, shape, axis)


def ones_where(cond):
    return jnp.where(cond, 1.0, 0.0).astype(BF16)


def fill(out_ref, mat, row_of, col_of, keep, product=dot):
    rows, cols = out_ref.shape
    depth = mat.shape[1] if product is dot else mat.shape[0]
    wide = product(mat, ones_where(iota((depth, cols), 0) == col_of(iota((depth, cols), 1)))).astype(BF16)
    for r0 in range(0, rows, L):
        p = iota((L, wide.shape[0]), 0) + r0
        block = dot(ones_where(iota((L, wide.shape[0]), 1) == row_of(p)), wide)
        same = keep(iota((L, cols), 0) + r0, iota((L, cols), 1))
        out_ref[r0:r0 + L, :] = jnp.where(same, block, 0.0).astype(BF16)


def alike(n):
    return lambda p, q: lax.rem(p, n) == lax.rem(q, n)


def compress_body(x_hbm, a1_hbm, a2_hbm, a3_hbm, b1_hbm, b2_hbm, b3_hbm, d_hbm, v2_out, l1_out,
                  fac, d_ref, xl, xr, u1o, u1s, u1r, k1o, k1r, k2o, k2r, k3, l3, l2, u2s, u2b, wbuf, dall, v3,
                  near_sem, xs_sem, xr_sem, credit, u1_sem, late_s, late_r,
                  u2_s, u2_r, w_s, w_r, d_sem, in_sem):
    c = lax.axis_index("mx")
    y = lax.axis_index("my")
    z = lax.axis_index("mz")
    oc, oy, oz = 1 - c, 1 - y, 1 - z

    def flip(rel):
        return (lax.rem(c + rel // QUART, TWO), lax.rem(y + rel // TWO % TWO, TWO), lax.rem(z + rel % TWO, TWO))

    def beside(rel):
        return (lax.rem(c + rel // TWO, TWO), y, lax.rem(z + rel % TWO, TWO))

    def ids(dev):
        return dict(zip(("mx", "my", "mz"), dev))

    def send(src, dst, s_sem, r_sem, dev):
        return pltpu.make_async_remote_copy(src, dst, s_sem, r_sem, device_id=ids(dev), device_id_type=MESH)

    peer, in_x, in_y, diagonal = (oc, y, z), (c, oy, z), (c, y, oz), (c, oy, oz)

    barrier = pltpu.get_barrier_semaphore()
    for rel in DEVICES:
        pl.semaphore_signal(barrier, inc=1, device_id=ids(flip(rel)), device_id_type=MESH)

    def half_of(core, t):
        return x_hbm.at[:, pl.ds(TWO * t, TWO), pl.ds(core * M, M), :]

    def near(t):
        slot = lax.rem(t, NEAR)
        return pltpu.make_async_copy(half_of(c, t), xl.at[slot], near_sem.at[slot])

    def cross(t):
        slot = lax.rem(t, RING)
        return send(half_of(oc, t), xr.at[slot], xs_sem.at[slot], xr_sem.at[slot], peer)

    loads = [pltpu.make_async_copy(src, fac.at[n], in_sem.at[n])
             for n, src in enumerate((a1_hbm, a2_hbm, a3_hbm, b1_hbm, b2_hbm, b3_hbm))]
    loads.append(pltpu.make_async_copy(d_hbm, d_ref, in_sem.at[len(loads)]))
    for load in loads:
        load.start()
    a1_ref, a2_ref, a3_ref, b1_ref, b2_ref, b3_ref = (fac.at[n] for n in range(len(loads) - 1))
    pl.semaphore_wait(barrier, len(DEVICES))
    for t in range(AHEAD):
        cross(t).start()
    for t in range(NEAR - 1):
        near(t).start()

    for load in loads:
        load.wait()

    def slot_of(dev):
        return QUART * dev[0] + TWO * dev[1] + dev[2]

    dall[slot_of((c, y, z))] = d_ref[...].reshape(H * H, H).T

    def rows_one(p):
        return lax.rem(p // T + H * y, M)

    fill(k1o, a1_ref[...], rows_one, lambda q: c * N + q // T, alike(T))
    fill(k1r, a1_ref[...], rows_one, lambda q: oc * N + q // T, alike(T))

    my_slot = slot_of((c, y, z))

    def diag(rel):
        return send(dall.at[my_slot], dall.at[my_slot], d_sem.at[0], d_sem.at[1], flip(rel))

    for rel in DEVICES:
        diag(rel).start()

    def pack(ref, slot):
        parts = [jnp.concatenate([ref[slot, :, s, 0:T, :], ref[slot, :, s, T:M, :]], axis=-1).reshape(N * T, L)
                 for s in range(TWO)]
        return jnp.concatenate(parts, axis=1)

    def early(t):
        part = (pl.ds(TWO * t, TWO), pl.ds(0, EARLY * T))
        return send(u1s.at[part], u1r.at[part], u1_sem.at[0], u1_sem.at[1], in_x)

    def late(g, n):
        span = N // CHUNKS[g]
        part = (pl.ds(span * n, span), pl.ds(STARTS[g] * T, SIZES[g] * T))
        return send(u1s.at[part], u1r.at[part], late_s, late_r.at[g], in_x)

    @pl.loop(0, STEPS)
    def _(t):
        @pl.when(t + NEAR - 1 < STEPS)
        def _():
            near(t + NEAR - 1).start()

        @pl.when(t >= 1)
        def _():
            early(t - 1).start()

        for n in range(FILLERS):
            @pl.when(t == S * (n + 1) + 1)
            def _(n=n):
                late(C, n).start()

        near(t).wait()
        cross(t).wait_recv()
        acc = dot(k1o[...], pack(xl, lax.rem(t, NEAR))) + dot(k1r[...], pack(xr, lax.rem(t, RING)))
        u1 = acc.astype(BF16)
        for s in range(TWO):
            u1o[TWO * t + s] = u1[:H * T, s * L:(s + 1) * L]
            u1s[TWO * t + s] = u1[H * T:, s * L:(s + 1) * L]

        @pl.when(t < STEPS - RING)
        def _():
            pl.semaphore_signal(credit, inc=1, device_id=ids(peer), device_id_type=MESH)

        @pl.when(t + AHEAD >= RING)
        def _():
            cross(t + AHEAD - RING).wait_send()

        @pl.when((t + AHEAD >= RING) & (t + AHEAD < STEPS))
        def _():
            pl.semaphore_wait(credit, 1)

        @pl.when(t + AHEAD < STEPS)
        def _():
            cross(t + AHEAD).start()

    def depart(g, first=0):
        for n in range(first, CHUNKS[g]):
            late(g, n).start()

    early(STEPS - 1).start()
    depart(C, FILLERS)
    depart(D)
    for t in range(STEPS - RING + AHEAD, STEPS):
        cross(t).wait_send()

    fill(k2o, a2_ref[...], lambda p: p // T, lambda q: y * N + q // T, alike(T))
    fill(k2r, a2_ref[...], lambda p: p // T, lambda q: oy * N + q // T, alike(T))
    q = iota((L, N), 1)
    k_first = lax.rem(z + q // T % TWO, TWO) * N + lax.rem(c + q // M, TWO) * M + lax.rem(q, T)
    for half in range(TWO):
        sel = ones_where(iota((L, N), 0) == k_first + T * half)
        k3[half * M:(half + 1) * M, :] = dot(a3_ref[...], sel).astype(BF16)
    fill(l2, b2_ref[...], lambda p: y * N + p // S, lambda q: q // S, alike(S), dot_t)
    fill(l1_out, b1_ref[...], lambda p: c * N + p // S, lambda q: q // S, alike(S), dot_t)
    fill(l3, b3_ref[...], lambda p: z * N + p // L * T + lax.rem(p, T), lambda q: lax.rem(q, M),
         lambda p, q: lax.rem(p, L) // T == q // M, dot_t)

    def second(i, width):
        def side(ref):
            return jnp.concatenate(
                [ref[:, pl.ds(pl.multiple_of((i + s) * T, T), T), :].reshape(N * T, L) for s in range(width)], axis=1)

        own, got = side(u1o), side(u1r)
        part = M * T * width // TWO
        for r0 in range(0, M * T, part):
            out = dot(k2o[r0:r0 + part, :], own) + dot(k2r[r0:r0 + part, :], got)
            for s in range(width):
                u2s[i + s, r0:r0 + part, :] = out[:, s * L:(s + 1) * L].astype(BF16)

    def quarter(dev):
        return TWO * dev[0] + dev[2]

    mine = quarter((c, y, z))

    def inner(g, rel):
        dev = beside(rel)
        i_span = pl.ds(STARTS[g], SIZES[g])
        return send(u2s.at[i_span, pl.ds(quarter(dev) * L, L)], u2b.at[rel - 1, i_span],
                    u2_s, u2_r.at[g], dev)

    def all_second(g):
        if SIZES[g] >= TWO:
            @pl.loop(0, SIZES[g] // TWO)
            def _(n):
                second(STARTS[g] + TWO * n, TWO)
        if SIZES[g] % TWO:
            second(STARTS[g] + SIZES[g] - 1, 1)
        for rel in (1, QUART - 1, TWO):
            inner(g, rel).start()

    low = iota((M, L), 1) < N
    lane = iota((M, TWO * L), 1)

    def third(g):
        got = u2b.at[:, pl.ds(STARTS[g], SIZES[g])]
        send(got, got, u2_s, u2_r.at[g], peer).wait_recv()
        base = slot_of((y, c, 0))
        d = jnp.concatenate([dall[base], dall[base + 1]], axis=0)

        @pl.loop(0, SIZES[g] * QUART, unroll=QUART)
        def _(n):
            i = STARTS[g] + n // QUART
            jl = lax.rem(n, QUART)

            def column(s):
                row = pl.multiple_of((TWO * jl + s) * T, T)
                own = u2s[i, pl.ds(pl.multiple_of(mine * L + row, T), T), :]
                return jnp.concatenate([own] + [u2b[rel - 1, i, pl.ds(row, T), :] for rel in OTHERS], axis=0)

            out = dot(k3[...], jnp.concatenate([column(0), column(1)], axis=1))
            first, other = out[:M], out[M:]
            u3 = jnp.where(low, first[:, :L] + pltpu.roll(other[:, :L], N, 1),
                           pltpu.roll(first[:, L:], N, 1) + other[:, L:])
            at = i * T + S * z + TWO * jl
            even = jnp.sum(jnp.where(lane == at, d, 0.0), axis=1, keepdims=True)
            odd = jnp.sum(jnp.where(lane == at + 1, d, 0.0), axis=1, keepdims=True)
            w = jnp.where(low, even, odd) * u3.astype(BF16).astype(F32)
            wbuf[y * H + i, mine * QUART + jl] = w.astype(BF16)

    def share(g, kind, owner, dev):
        at = (pl.ds(owner[1] * H + STARTS[g], SIZES[g]), pl.ds(quarter(owner) * QUART, QUART))
        return send(wbuf.at[at], wbuf.at[at], w_s, w_r.at[g, BY_KIND[kind]], dev)

    OWN_X, OWN_Y, X_Y, OWN_P, Y_P, X_P, D_P = range(KINDS)
    SAME, OTHER = OWN_P, OWN_P + 1
    BY_KIND = (OWN_X, OWN_Y, X_Y, SAME, SAME, OTHER, OTHER)

    def gather_near(g):
        share(g, OWN_Y, (c, y, z), in_y).start()
        share(g, OWN_P, (c, y, z), peer).start()

    def gather_far(g):
        share(g, OWN_X, (c, y, z), in_x).start()
        if g in DIRECT:
            share(g, X_Y, (c, y, z), diagonal).start()

    def forward_near(g):
        share(g, OWN_Y, in_y, in_y).wait_recv()
        share(g, Y_P, in_y, peer).start()

    def forward_far(g):
        share(g, OWN_X, in_x, in_x).wait_recv()
        if g not in DIRECT:
            share(g, X_Y, in_x, in_y).start()
        share(g, X_P, in_x, peer).start()

    def forward_diagonal(g):
        share(g, X_Y, diagonal, in_y).wait_recv()
        share(g, D_P, diagonal, peer).start()

    def gathered(g, side):
        got = wbuf.at[pl.ds(0, SIZES[g]), pl.ds(0, TWO * QUART)]
        send(got, got, w_s, w_r.at[g, side], peer).wait_recv()

    low_v = iota((QUART, S, S, L), TWO + 1) < N

    def middle(i0):
        for jo in range(TWO):
            rhs = jnp.concatenate(
                [wbuf[i0 + s, jo * S:(jo + 1) * S].reshape(TWO * L, L) for s in range(TWO)], axis=1)
            out = dot(l3[...], rhs)
            for s in range(TWO):
                o = out[:, s * L:(s + 1) * L].reshape(QUART, S, TWO, S, L)
                t0, t1 = o[:, :, 0], o[:, :, 1]
                even = jnp.where(low_v, t0, pltpu.roll(t1, N, TWO + 1))
                odd = jnp.where(low_v, pltpu.roll(t0, N, TWO + 1), t1)
                both = jnp.concatenate([even, odd], axis=TWO).astype(BF16)
                v3[:, s, jo * L:(jo + 1) * L, :] = both.reshape(QUART, L, L)
        for kb in range(QUART):
            out = dot(l2[...], jnp.concatenate([v3[kb, 0], v3[kb, 1]], axis=1))
            pair = jnp.concatenate([out[:, :L].reshape(N, S, L), out[:, L:].reshape(N, S, L)], axis=1)
            v2_out[kb, :, pl.ds(pl.multiple_of(i0 * S, T), T), :] = pair.astype(BF16)

    def near_middle(g):
        @pl.loop(0, max(SIZES[g] // TWO, 1))
        def _(n):
            middle(y * H + STARTS[g] + TWO * n)

    def far_middle(g):
        @pl.loop(0, max(SIZES[g] // TWO, 1))
        def _(n):
            middle(oy * H + STARTS[g] + TWO * n)

    def near_end(g):
        gathered(g, SAME)

    def far_end(g):
        gathered(g, OTHER)

    def arrived(g):
        got = u1r.at[:, pl.ds(STARTS[g] * T, SIZES[g] * T)]
        send(got, got, late_s, late_r.at[g], in_x).wait_recv()

    first = u1r.at[:, pl.ds(0, EARLY * T)]
    rest = u1r.at[:, pl.ds(EARLY * T, EARLY * T)]
    cores = dall.at[pl.ds(0, len(DEVICES))]
    send(first, first, u1_sem.at[0], u1_sem.at[1], in_x).wait_recv()
    send(cores, cores, d_sem.at[0], d_sem.at[1], peer).wait_recv()
    all_second(A)
    all_second(B)
    arrived(C)
    all_second(C)
    third(A)
    gather_near(A)
    gather_far(A)
    third(B)
    gather_near(B)
    gather_far(B)
    depart(E)
    third(C)
    gather_near(C)
    gather_far(C)
    depart(F)
    depart(G)
    arrived(D)
    all_second(D)
    forward_near(A)
    forward_far(A)
    near_end(A)
    near_middle(A)
    forward_near(B)
    forward_far(B)
    near_end(B)
    near_middle(B)
    forward_near(C)
    third(D)
    gather_near(D)
    gather_far(D)
    forward_diagonal(A)
    far_end(A)
    far_middle(A)
    forward_diagonal(B)
    near_end(C)
    near_middle(C)
    arrived(E)
    all_second(E)
    forward_far(C)
    forward_near(D)
    far_end(B)
    far_middle(B)
    near_end(D)
    near_middle(D)
    arrived(F)
    all_second(F)
    third(E)
    gather_near(E)
    gather_far(E)
    forward_diagonal(C)
    far_end(C)
    far_middle(C)
    third(F)
    gather_near(F)
    gather_far(F)
    arrived(G)
    all_second(G)
    forward_near(E)
    near_end(E)
    near_middle(E)
    forward_far(D)
    forward_near(F)
    forward_far(E)
    third(G)
    gather_near(G)
    gather_far(G)
    forward_diagonal(D)
    forward_far(F)
    forward_diagonal(E)
    far_end(D)
    far_middle(D)
    forward_near(G)
    forward_diagonal(F)
    forward_far(G)
    forward_diagonal(G)
    near_end(F)
    near_end(G)
    near_middle(F)
    far_end(E)
    far_middle(E)
    far_end(F)
    far_end(G)
    far_middle(F)

    sent = wbuf.at[pl.ds(0, KINDS * QUART), :]
    send(first, first, u1_sem.at[0], u1_sem.at[1], in_x).wait_send()
    send(rest, rest, late_s, late_r.at[0], in_x).wait_send()
    send(cores, cores, d_sem.at[0], d_sem.at[1], peer).wait_send()
    send(u2b, u2b, u2_s, u2_r.at[0], peer).wait_send()
    send(sent, sent, w_s, w_r.at[0, 0], peer).wait_send()


def compress(x, a1, a2, a3, b1_t, b2_t, b3_t, d):
    vmem = pl.BlockSpec(memory_space=pltpu.VMEM)
    hbm = pl.BlockSpec(memory_space=pltpu.HBM)
    dma = pltpu.SemaphoreType.DMA
    u1 = pltpu.VMEM((N, H * T, L), BF16)
    spread = pltpu.VMEM((M * T, N * T), BF16)
    groups = len(SIZES)
    return pl.pallas_call(
        compress_body,
        out_shape=(pltpu.VMEM((QUART, N, M * S, L), BF16), pltpu.VMEM((N * S, M * S), BF16)),
        in_specs=[hbm] * 8,
        out_specs=(vmem, vmem),
        scratch_shapes=[
            pltpu.VMEM((6, M, L), BF16), pltpu.VMEM((H, H, H), F32),
            pltpu.VMEM((NEAR, N, TWO, M, N), BF16), pltpu.VMEM((RING, N, TWO, M, N), BF16), u1, u1, u1,
            spread, spread, spread, spread, pltpu.VMEM((N, N), BF16),
            pltpu.VMEM((M * T, M * S), BF16), pltpu.VMEM((N * S, M * S), BF16),
            pltpu.VMEM((H, M * T, L), BF16), pltpu.VMEM((len(OTHERS), H, L, L), BF16),
            pltpu.VMEM((M, H, M, L), BF16), pltpu.VMEM((S, H, H * H), F32),
            pltpu.VMEM((QUART, TWO, M * S, L), BF16),
            dma((NEAR,)), dma((RING,)), dma((RING,)), pltpu.SemaphoreType.REGULAR,
            dma((TWO,)), dma, dma((groups,)), dma, dma((groups,)), dma, dma((groups, QUART + 1)), dma((TWO,)), dma((KINDS,)),
        ],
        compiler_params=pltpu.CompilerParams(collective_id=0, has_side_effects=True, vmem_limit_bytes=LIMIT),
        name="compress",
    )(x, a1, a2, a3, b1_t, b2_t, b3_t, d)


def expand_body(v2_ref, l1_ref, z_hbm, zbuf, z_sem):
    per_block = N // COLUMNS

    def leave(n):
        slot = lax.rem(n, SLOTS)
        where = (slice(None), pl.ds(n % per_block * COLUMNS, COLUMNS), pl.ds(n // per_block * T, T))
        return pltpu.make_async_copy(zbuf.at[slot], z_hbm.at[where], z_sem.at[slot])

    @pl.loop(0, QUART * per_block)
    def _(n):
        slot = lax.rem(n, SLOTS)

        @pl.when(n >= SLOTS)
        def _():
            leave(n - SLOTS).wait()

        for j in range(0, COLUMNS, TWO):
            at = n % per_block * COLUMNS + j
            out = dot(l1_ref[...], jnp.concatenate([v2_ref[n // per_block, at + s] for s in range(TWO)], axis=1))
            for s in range(TWO):
                o = out[:, s * L:(s + 1) * L].reshape(N, S, L)
                zbuf[slot, :, j + s, :S, :] = o[:, :, :N]
                zbuf[slot, :, j + s, S:, :] = pltpu.roll(o, N, TWO)[:, :, :N]
        leave(n).start()

    for n in range(QUART * per_block - SLOTS, QUART * per_block):
        leave(n).wait()


def expand(v2, l1):
    vmem = pl.BlockSpec(memory_space=pltpu.VMEM)
    return pl.pallas_call(
        expand_body,
        out_shape=jax.ShapeDtypeStruct((N, N, N, N), F32),
        in_specs=[vmem, vmem],
        out_specs=pl.BlockSpec(memory_space=pl.ANY),
        scratch_shapes=[pltpu.VMEM((SLOTS, N, COLUMNS, T, N), F32), pltpu.SemaphoreType.DMA((SLOTS,))],
        compiler_params=pltpu.CompilerParams(vmem_limit_bytes=LIMIT // 2),
        name="expand",
    )(v2, l1)


def solution(mesh):
    vol_spec = P("mx", "my", "mz", "rhs")
    core_spec = P("mx", "my", "mz")
    full_spec = P()

    def local_operator(x_blk, fac_a1, fac_a2, fac_a3, diag_blk, fac_b1, fac_b2, fac_b3):
        v2, l1 = compress(x_blk, fac_a1, fac_a2, fac_a3, fac_b1.T, fac_b2.T, fac_b3.T, diag_blk)
        return expand(v2, l1)

    return jax.shard_map(local_operator, mesh=mesh, in_specs=(vol_spec, full_spec, full_spec, full_spec, core_spec, full_spec, full_spec, full_spec), out_specs=vol_spec, check_vma=False)
```

```python
import jax
import jax.numpy as jnp
from jax import lax
from jax.experimental import pallas as pl
from jax.experimental.pallas import tpu as pltpu
from jax.sharding import PartitionSpec as P

F32 = jnp.float32
BF16 = jnp.bfloat16
MESH = pl.DeviceIdType.MESH
N = 64
M = 32
L = 128
T = 16
S = 8
TWO = 2
QUART = 4
H = M // TWO
RING = 8
AHEAD = 4
NEAR = 4
STEPS = N // TWO
EARLY = 8
A, B, C, D, E, F, G = range(7)
SIZES = (4, 4, 2, 2, 2, 1, 1)
STARTS = (0, 4, 8, 10, 12, 14, 15)
CHUNKS = (0, 0, 8, 2, 2, 1, 1)
DIRECT = (F, G)
FILLERS = 4
GROUPS = range(len(SIZES))
OTHERS = range(1, QUART)
DEVICES = range(1, S)
KINDS = 7
COLUMNS = 4
SLOTS = 4
LIMIT = 42 * 1024 * 1024


def dot(a, b):
    return jnp.dot(a, b, preferred_element_type=F32)


def dot_t(a, b):
    return lax.dot_general(a, b, (((0,), (0,)), ((), ())), preferred_element_type=F32)


def iota(shape, axis):
    return lax.broadcasted_iota(jnp.int32, shape, axis)


def ones_where(cond):
    return jnp.where(cond, 1.0, 0.0).astype(BF16)


def fill(out_ref, mat, row_of, col_of, keep, product=dot):
    rows, cols = out_ref.shape
    depth = mat.shape[1] if product is dot else mat.shape[0]
    wide = product(mat, ones_where(iota((depth, cols), 0) == col_of(iota((depth, cols), 1)))).astype(BF16)
    for r0 in range(0, rows, L):
        p = iota((L, wide.shape[0]), 0) + r0
        block = dot(ones_where(iota((L, wide.shape[0]), 1) == row_of(p)), wide)
        same = keep(iota((L, cols), 0) + r0, iota((L, cols), 1))
        out_ref[r0:r0 + L, :] = jnp.where(same, block, 0.0).astype(BF16)


def alike(n):
    return lambda p, q: lax.rem(p, n) == lax.rem(q, n)


def compress_body(x_hbm, a1_hbm, a2_hbm, a3_hbm, b1_hbm, b2_hbm, b3_hbm, d_hbm, v2_out, l1_out,
                  fac, d_ref, xl, xr, u1o, u1s, u1r, k1o, k1r, k2o, k2r, k3, l3, l2, u2s, u2b, wbuf, dall, v3,
                  near_sem, xs_sem, xr_sem, credit, u1_sem, late_s, late_r,
                  u2_s, u2_r, w_s, w_r, d_sem, in_sem):
    c = lax.axis_index("mx")
    y = lax.axis_index("my")
    z = lax.axis_index("mz")
    oc, oy, oz = 1 - c, 1 - y, 1 - z

    def flip(rel):
        return (lax.rem(c + rel // QUART, TWO), lax.rem(y + rel // TWO % TWO, TWO), lax.rem(z + rel % TWO, TWO))

    def beside(rel):
        return (lax.rem(c + rel // TWO, TWO), y, lax.rem(z + rel % TWO, TWO))

    def ids(dev):
        return dict(zip(("mx", "my", "mz"), dev))

    def send(src, dst, s_sem, r_sem, dev):
        return pltpu.make_async_remote_copy(src, dst, s_sem, r_sem, device_id=ids(dev), device_id_type=MESH)

    peer, in_x, in_y, diagonal = (oc, y, z), (c, oy, z), (c, y, oz), (c, oy, oz)

    barrier = pltpu.get_barrier_semaphore()
    for rel in DEVICES:
        pl.semaphore_signal(barrier, inc=1, device_id=ids(flip(rel)), device_id_type=MESH)

    def half_of(core, t):
        return x_hbm.at[:, pl.ds(TWO * t, TWO), pl.ds(core * M, M), :]

    def near(t):
        slot = lax.rem(t, NEAR)
        return pltpu.make_async_copy(half_of(c, t), xl.at[slot], near_sem.at[slot])

    def cross(t):
        slot = lax.rem(t, RING)
        return send(half_of(oc, t), xr.at[slot], xs_sem.at[slot], xr_sem.at[slot], peer)

    loads = [pltpu.make_async_copy(src, fac.at[n], in_sem.at[n])
             for n, src in enumerate((a1_hbm, a2_hbm, a3_hbm, b1_hbm, b2_hbm, b3_hbm))]
    loads.append(pltpu.make_async_copy(d_hbm, d_ref, in_sem.at[len(loads)]))
    for load in loads:
        load.start()
    a1_ref, a2_ref, a3_ref, b1_ref, b2_ref, b3_ref = (fac.at[n] for n in range(len(loads) - 1))
    pl.semaphore_wait(barrier, len(DEVICES))
    for t in range(AHEAD):
        cross(t).start()
    for t in range(NEAR - 1):
        near(t).start()

    for load in loads:
        load.wait()

    def slot_of(dev):
        return QUART * dev[0] + TWO * dev[1] + dev[2]

    dall[slot_of((c, y, z))] = d_ref[...].reshape(H * H, H).T

    def rows_one(p):
        return lax.rem(p // T + H * y, M)

    fill(k1o, a1_ref[...], rows_one, lambda q: c * N + q // T, alike(T))
    fill(k1r, a1_ref[...], rows_one, lambda q: oc * N + q // T, alike(T))

    my_slot = slot_of((c, y, z))

    def diag(rel):
        return send(dall.at[my_slot], dall.at[my_slot], d_sem.at[0], d_sem.at[1], flip(rel))

    for rel in DEVICES:
        diag(rel).start()

    def pack(ref, slot):
        parts = [jnp.concatenate([ref[slot, :, s, 0:T, :], ref[slot, :, s, T:M, :]], axis=-1).reshape(N * T, L)
                 for s in range(TWO)]
        return jnp.concatenate(parts, axis=1)

    def early(t):
        part = (pl.ds(TWO * t, TWO), pl.ds(0, EARLY * T))
        return send(u1s.at[part], u1r.at[part], u1_sem.at[0], u1_sem.at[1], in_x)

    def late(g, n):
        span = N // CHUNKS[g]
        part = (pl.ds(span * n, span), pl.ds(STARTS[g] * T, SIZES[g] * T))
        return send(u1s.at[part], u1r.at[part], late_s, late_r.at[g], in_x)

    @pl.loop(0, STEPS)
    def _(t):
        @pl.when(t + NEAR - 1 < STEPS)
        def _():
            near(t + NEAR - 1).start()

        @pl.when(t >= 1)
        def _():
            early(t - 1).start()

        for n in range(FILLERS):
            @pl.when(t == QUART * (n + 1) + 1)
            def _(n=n):
                late(C, n).start()

        near(t).wait()
        cross(t).wait_recv()
        acc = dot(k1o[...], pack(xl, lax.rem(t, NEAR))) + dot(k1r[...], pack(xr, lax.rem(t, RING)))
        u1 = acc.astype(BF16)
        for s in range(TWO):
            u1o[TWO * t + s] = u1[:H * T, s * L:(s + 1) * L]
            u1s[TWO * t + s] = u1[H * T:, s * L:(s + 1) * L]

        @pl.when(t < STEPS - RING)
        def _():
            pl.semaphore_signal(credit, inc=1, device_id=ids(peer), device_id_type=MESH)

        @pl.when(t + AHEAD >= RING)
        def _():
            cross(t + AHEAD - RING).wait_send()

        @pl.when((t + AHEAD >= RING) & (t + AHEAD < STEPS))
        def _():
            pl.semaphore_wait(credit, 1)

        @pl.when(t + AHEAD < STEPS)
        def _():
            cross(t + AHEAD).start()

    def depart(g, first=0):
        for n in range(first, CHUNKS[g]):
            late(g, n).start()

    early(STEPS - 1).start()
    depart(C, FILLERS)
    depart(D)
    for t in range(STEPS - RING + AHEAD, STEPS):
        cross(t).wait_send()

    fill(k2o, a2_ref[...], lambda p: p // T, lambda q: y * N + q // T, alike(T))
    fill(k2r, a2_ref[...], lambda p: p // T, lambda q: oy * N + q // T, alike(T))
    q = iota((L, N), 1)
    k_first = lax.rem(z + q // T % TWO, TWO) * N + lax.rem(c + q // M, TWO) * M + lax.rem(q, T)
    for half in range(TWO):
        sel = ones_where(iota((L, N), 0) == k_first + T * half)
        k3[half * M:(half + 1) * M, :] = dot(a3_ref[...], sel).astype(BF16)
    fill(l2, b2_ref[...], lambda p: y * N + p // S, lambda q: q // S, alike(S), dot_t)
    fill(l1_out, b1_ref[...], lambda p: c * N + p // S, lambda q: q // S, alike(S), dot_t)
    fill(l3, b3_ref[...], lambda p: z * N + p // L * T + lax.rem(p, T), lambda q: lax.rem(q, M),
         lambda p, q: lax.rem(p, L) // T == q // M, dot_t)

    def second(i, width):
        def side(ref):
            return jnp.concatenate(
                [ref[:, pl.ds(pl.multiple_of((i + s) * T, T), T), :].reshape(N * T, L) for s in range(width)], axis=1)

        own, got = side(u1o), side(u1r)
        part = M * T * width // TWO
        for r0 in range(0, M * T, part):
            out = dot(k2o[r0:r0 + part, :], own) + dot(k2r[r0:r0 + part, :], got)
            for s in range(width):
                u2s[i + s, r0:r0 + part, :] = out[:, s * L:(s + 1) * L].astype(BF16)

    def quarter(dev):
        return TWO * dev[0] + dev[2]

    mine = quarter((c, y, z))

    def inner(g, rel):
        dev = beside(rel)
        i_span = pl.ds(STARTS[g], SIZES[g])
        return send(u2s.at[i_span, pl.ds(quarter(dev) * L, L)], u2b.at[rel - 1, i_span],
                    u2_s, u2_r.at[g], dev)

    def all_second(g):
        if SIZES[g] >= TWO:
            @pl.loop(0, SIZES[g] // TWO)
            def _(n):
                second(STARTS[g] + TWO * n, TWO)
        if SIZES[g] % TWO:
            second(STARTS[g] + SIZES[g] - 1, 1)
        for rel in (1, QUART - 1, TWO):
            inner(g, rel).start()

    low = iota((M, L), 1) < N
    lane = iota((M, TWO * L), 1)

    def third(g):
        got = u2b.at[:, pl.ds(STARTS[g], SIZES[g])]
        send(got, got, u2_s, u2_r.at[g], peer).wait_recv()
        base = slot_of((y, c, 0))
        d = jnp.concatenate([dall[base], dall[base + 1]], axis=0)

        @pl.loop(0, SIZES[g] * QUART, unroll=QUART)
        def _(n):
            i = STARTS[g] + n // QUART
            jl = lax.rem(n, QUART)

            def column(s):
                row = pl.multiple_of((TWO * jl + s) * T, T)
                own = u2s[i, pl.ds(pl.multiple_of(mine * L + row, T), T), :]
                return jnp.concatenate([own] + [u2b[rel - 1, i, pl.ds(row, T), :] for rel in OTHERS], axis=0)

            out = dot(k3[...], jnp.concatenate([column(0), column(1)], axis=1))
            first, other = out[:M], out[M:]
            u3 = jnp.where(low, first[:, :L] + pltpu.roll(other[:, :L], N, 1),
                           pltpu.roll(first[:, L:], N, 1) + other[:, L:])
            at = i * T + S * z + TWO * jl
            even = jnp.sum(jnp.where(lane == at, d, 0.0), axis=1, keepdims=True)
            odd = jnp.sum(jnp.where(lane == at + 1, d, 0.0), axis=1, keepdims=True)
            w = jnp.where(low, even, odd) * u3.astype(BF16).astype(F32)
            wbuf[y * H + i, mine * QUART + jl] = w.astype(BF16)

    def share(g, kind, owner, dev):
        at = (pl.ds(owner[1] * H + STARTS[g], SIZES[g]), pl.ds(quarter(owner) * QUART, QUART))
        return send(wbuf.at[at], wbuf.at[at], w_s, w_r.at[g, BY_KIND[kind]], dev)

    OWN_X, OWN_Y, X_Y, OWN_P, Y_P, X_P, D_P = range(KINDS)
    SAME, OTHER = OWN_P, OWN_P + 1
    BY_KIND = (OWN_X, OWN_Y, X_Y, SAME, SAME, OTHER, OTHER)

    def gather_near(g):
        share(g, OWN_Y, (c, y, z), in_y).start()
        share(g, OWN_P, (c, y, z), peer).start()

    def gather_far(g):
        share(g, OWN_X, (c, y, z), in_x).start()
        if g in DIRECT:
            share(g, X_Y, (c, y, z), diagonal).start()

    def forward_near(g):
        share(g, OWN_Y, in_y, in_y).wait_recv()
        share(g, Y_P, in_y, peer).start()

    def forward_far(g):
        share(g, OWN_X, in_x, in_x).wait_recv()
        if g not in DIRECT:
            share(g, X_Y, in_x, in_y).start()
        share(g, X_P, in_x, peer).start()

    def forward_diagonal(g):
        share(g, X_Y, diagonal, in_y).wait_recv()
        share(g, D_P, diagonal, peer).start()

    def gathered(g, side):
        got = wbuf.at[pl.ds(0, SIZES[g]), pl.ds(0, TWO * QUART)]
        send(got, got, w_s, w_r.at[g, side], peer).wait_recv()

    low_v = iota((QUART, S, S, L), TWO + 1) < N

    def middle(i0):
        for jo in range(TWO):
            rhs = jnp.concatenate(
                [wbuf[i0 + s, jo * S:(jo + 1) * S].reshape(TWO * L, L) for s in range(TWO)], axis=1)
            out = dot(l3[...], rhs)
            for s in range(TWO):
                o = out[:, s * L:(s + 1) * L].reshape(QUART, S, TWO, S, L)
                t0, t1 = o[:, :, 0], o[:, :, 1]
                even = jnp.where(low_v, t0, pltpu.roll(t1, N, TWO + 1))
                odd = jnp.where(low_v, pltpu.roll(t0, N, TWO + 1), t1)
                both = jnp.concatenate([even, odd], axis=TWO).astype(BF16)
                v3[:, s, jo * L:(jo + 1) * L, :] = both.reshape(QUART, L, L)
        for kb in range(QUART):
            out = dot(l2[...], jnp.concatenate([v3[kb, 0], v3[kb, 1]], axis=1))
            pair = jnp.concatenate([out[:, :L].reshape(N, S, L), out[:, L:].reshape(N, S, L)], axis=1)
            v2_out[kb, :, pl.ds(pl.multiple_of(i0 * S, T), T), :] = pair.astype(BF16)

    def near_middle(g):
        @pl.loop(0, max(SIZES[g] // TWO, 1))
        def _(n):
            middle(y * H + STARTS[g] + TWO * n)

    def far_middle(g):
        @pl.loop(0, max(SIZES[g] // TWO, 1))
        def _(n):
            middle(oy * H + STARTS[g] + TWO * n)

    def near_end(g):
        gathered(g, SAME)

    def far_end(g):
        gathered(g, OTHER)

    def arrived(g):
        got = u1r.at[:, pl.ds(STARTS[g] * T, SIZES[g] * T)]
        send(got, got, late_s, late_r.at[g], in_x).wait_recv()

    first = u1r.at[:, pl.ds(0, EARLY * T)]
    rest = u1r.at[:, pl.ds(EARLY * T, EARLY * T)]
    cores = dall.at[pl.ds(0, len(DEVICES))]
    send(first, first, u1_sem.at[0], u1_sem.at[1], in_x).wait_recv()
    send(cores, cores, d_sem.at[0], d_sem.at[1], peer).wait_recv()
    all_second(A)
    all_second(B)
    arrived(C)
    all_second(C)
    third(A)
    gather_near(A)
    gather_far(A)
    third(B)
    gather_near(B)
    gather_far(B)
    depart(E)
    third(C)
    gather_near(C)
    gather_far(C)
    depart(F)
    depart(G)
    arrived(D)
    all_second(D)
    forward_near(A)
    forward_far(A)
    near_end(A)
    near_middle(A)
    forward_near(B)
    forward_far(B)
    near_end(B)
    near_middle(B)
    forward_near(C)
    third(D)
    gather_near(D)
    gather_far(D)
    forward_diagonal(A)
    far_end(A)
    far_middle(A)
    forward_diagonal(B)
    near_end(C)
    near_middle(C)
    arrived(E)
    all_second(E)
    forward_far(C)
    forward_near(D)
    far_end(B)
    far_middle(B)
    near_end(D)
    near_middle(D)
    arrived(F)
    all_second(F)
    third(E)
    gather_near(E)
    gather_far(E)
    forward_diagonal(C)
    far_end(C)
    far_middle(C)
    third(F)
    gather_near(F)
    gather_far(F)
    arrived(G)
    all_second(G)
    forward_near(E)
    near_end(E)
    near_middle(E)
    forward_far(D)
    forward_near(F)
    forward_far(E)
    third(G)
    gather_near(G)
    gather_far(G)
    forward_diagonal(D)
    forward_far(F)
    forward_diagonal(E)
    far_end(D)
    far_middle(D)
    forward_near(G)
    forward_diagonal(F)
    forward_far(G)
    forward_diagonal(G)
    near_end(F)
    near_end(G)
    near_middle(F)
    far_end(E)
    far_middle(E)
    far_end(F)
    far_end(G)
    far_middle(F)

    sent = wbuf.at[pl.ds(0, KINDS * QUART), :]
    send(first, first, u1_sem.at[0], u1_sem.at[1], in_x).wait_send()
    send(rest, rest, late_s, late_r.at[0], in_x).wait_send()
    send(cores, cores, d_sem.at[0], d_sem.at[1], peer).wait_send()
    send(u2b, u2b, u2_s, u2_r.at[0], peer).wait_send()
    send(sent, sent, w_s, w_r.at[0, 0], peer).wait_send()


def compress(x, a1, a2, a3, b1_t, b2_t, b3_t, d):
    vmem = pl.BlockSpec(memory_space=pltpu.VMEM)
    hbm = pl.BlockSpec(memory_space=pltpu.HBM)
    dma = pltpu.SemaphoreType.DMA
    u1 = pltpu.VMEM((N, H * T, L), BF16)
    spread = pltpu.VMEM((M * T, N * T), BF16)
    groups = len(SIZES)
    return pl.pallas_call(
        compress_body,
        out_shape=(pltpu.VMEM((QUART, N, M * S, L), BF16), pltpu.VMEM((N * S, M * S), BF16)),
        in_specs=[hbm] * 8,
        out_specs=(vmem, vmem),
        scratch_shapes=[
            pltpu.VMEM((6, M, L), BF16), pltpu.VMEM((H, H, H), F32),
            pltpu.VMEM((NEAR, N, TWO, M, N), BF16), pltpu.VMEM((RING, N, TWO, M, N), BF16), u1, u1, u1,
            spread, spread, spread, spread, pltpu.VMEM((N, N), BF16),
            pltpu.VMEM((M * T, M * S), BF16), pltpu.VMEM((N * S, M * S), BF16),
            pltpu.VMEM((H, M * T, L), BF16), pltpu.VMEM((len(OTHERS), H, L, L), BF16),
            pltpu.VMEM((M, H, M, L), BF16), pltpu.VMEM((S, H, H * H), F32),
            pltpu.VMEM((QUART, TWO, M * S, L), BF16),
            dma((NEAR,)), dma((RING,)), dma((RING,)), pltpu.SemaphoreType.REGULAR,
            dma((TWO,)), dma, dma((groups,)), dma, dma((groups,)), dma, dma((groups, QUART + 1)), dma((TWO,)), dma((KINDS,)),
        ],
        compiler_params=pltpu.CompilerParams(collective_id=0, has_side_effects=True, vmem_limit_bytes=LIMIT),
        name="compress",
    )(x, a1, a2, a3, b1_t, b2_t, b3_t, d)


def expand_body(v2_ref, l1_ref, z_hbm, zbuf, z_sem):
    per_block = N // COLUMNS

    def leave(n):
        slot = lax.rem(n, SLOTS)
        where = (slice(None), pl.ds(n % per_block * COLUMNS, COLUMNS), pl.ds(n // per_block * T, T))
        return pltpu.make_async_copy(zbuf.at[slot], z_hbm.at[where], z_sem.at[slot])

    @pl.loop(0, QUART * per_block)
    def _(n):
        slot = lax.rem(n, SLOTS)

        @pl.when(n >= SLOTS)
        def _():
            leave(n - SLOTS).wait()

        for j in range(0, COLUMNS, TWO):
            at = n % per_block * COLUMNS + j
            out = dot(l1_ref[...], jnp.concatenate([v2_ref[n // per_block, at + s] for s in range(TWO)], axis=1))
            for s in range(TWO):
                o = out[:, s * L:(s + 1) * L].reshape(N, S, L)
                zbuf[slot, :, j + s, :S, :] = o[:, :, :N]
                zbuf[slot, :, j + s, S:, :] = pltpu.roll(o, N, TWO)[:, :, :N]
        leave(n).start()

    for n in range(QUART * per_block - SLOTS, QUART * per_block):
        leave(n).wait()


def expand(v2, l1):
    vmem = pl.BlockSpec(memory_space=pltpu.VMEM)
    return pl.pallas_call(
        expand_body,
        out_shape=jax.ShapeDtypeStruct((N, N, N, N), F32),
        in_specs=[vmem, vmem],
        out_specs=pl.BlockSpec(memory_space=pl.ANY),
        scratch_shapes=[pltpu.VMEM((SLOTS, N, COLUMNS, T, N), F32), pltpu.SemaphoreType.DMA((SLOTS,))],
        compiler_params=pltpu.CompilerParams(vmem_limit_bytes=LIMIT // 2),
        name="expand",
    )(v2, l1)


def solution(mesh):
    vol_spec = P("mx", "my", "mz", "rhs")
    core_spec = P("mx", "my", "mz")
    full_spec = P()

    def local_operator(x_blk, fac_a1, fac_a2, fac_a3, diag_blk, fac_b1, fac_b2, fac_b3):
        v2, l1 = compress(x_blk, fac_a1, fac_a2, fac_a3, fac_b1.T, fac_b2.T, fac_b3.T, diag_blk)
        return expand(v2, l1)

    return jax.shard_map(local_operator, mesh=mesh, in_specs=(vol_spec, full_spec, full_spec, full_spec, core_spec, full_spec, full_spec, full_spec), out_specs=vol_spec, check_vma=False)
```

```python
import jax
import jax.numpy as jnp
from jax import lax
from jax.experimental import pallas as pl
from jax.experimental.pallas import tpu as pltpu
from jax.sharding import PartitionSpec as P

F32 = jnp.float32
BF16 = jnp.bfloat16
MESH = pl.DeviceIdType.MESH
N = 64
M = 32
L = 128
T = 16
S = 8
TWO = 2
QUART = 4
H = M // TWO
RING = 8
AHEAD = 4
NEAR = 4
STEPS = N // TWO
EARLY = 8
A, B, C, D, E, F, G = range(7)
SIZES = (4, 4, 2, 2, 2, 1, 1)
STARTS = (0, 4, 8, 10, 12, 14, 15)
CHUNKS = (0, 0, 8, 2, 2, 1, 1)
DIRECT = (F, G)
FILLERS = 4
GROUPS = range(len(SIZES))
OTHERS = range(1, QUART)
DEVICES = range(1, S)
KINDS = 7
COLUMNS = 4
SLOTS = 4
LIMIT = 42 * 1024 * 1024


def dot(a, b):
    return jnp.dot(a, b, preferred_element_type=F32)


def dot_t(a, b):
    return lax.dot_general(a, b, (((0,), (0,)), ((), ())), preferred_element_type=F32)


def iota(shape, axis):
    return lax.broadcasted_iota(jnp.int32, shape, axis)


def ones_where(cond):
    return jnp.where(cond, 1.0, 0.0).astype(BF16)


def fill(out_ref, mat, row_of, col_of, keep, product=dot):
    rows, cols = out_ref.shape
    depth = mat.shape[1] if product is dot else mat.shape[0]
    wide = product(mat, ones_where(iota((depth, cols), 0) == col_of(iota((depth, cols), 1)))).astype(BF16)
    for r0 in range(0, rows, L):
        p = iota((L, wide.shape[0]), 0) + r0
        block = dot(ones_where(iota((L, wide.shape[0]), 1) == row_of(p)), wide)
        same = keep(iota((L, cols), 0) + r0, iota((L, cols), 1))
        out_ref[r0:r0 + L, :] = jnp.where(same, block, 0.0).astype(BF16)


def alike(n):
    return lambda p, q: lax.rem(p, n) == lax.rem(q, n)


def compress_body(x_hbm, a1_hbm, a2_hbm, a3_hbm, b1_hbm, b2_hbm, b3_hbm, d_hbm, v2_out, l1_out,
                  fac, d_ref, xl, xr, u1o, u1s, u1r, k1o, k1r, k2o, k2r, k3, l3, l2, u2s, u2b, wbuf, dall, v3,
                  near_sem, xs_sem, xr_sem, credit, u1_sem, late_s, late_r,
                  u2_s, u2_r, w_s, w_r, d_sem, in_sem):
    c = lax.axis_index("mx")
    y = lax.axis_index("my")
    z = lax.axis_index("mz")
    oc, oy, oz = 1 - c, 1 - y, 1 - z

    def flip(rel):
        return (lax.rem(c + rel // QUART, TWO), lax.rem(y + rel // TWO % TWO, TWO), lax.rem(z + rel % TWO, TWO))

    def beside(rel):
        return (lax.rem(c + rel // TWO, TWO), y, lax.rem(z + rel % TWO, TWO))

    def ids(dev):
        return dict(zip(("mx", "my", "mz"), dev))

    def send(src, dst, s_sem, r_sem, dev):
        return pltpu.make_async_remote_copy(src, dst, s_sem, r_sem, device_id=ids(dev), device_id_type=MESH)

    peer, in_x, in_y, diagonal = (oc, y, z), (c, oy, z), (c, y, oz), (c, oy, oz)

    barrier = pltpu.get_barrier_semaphore()
    for rel in DEVICES:
        pl.semaphore_signal(barrier, inc=1, device_id=ids(flip(rel)), device_id_type=MESH)

    def half_of(core, t):
        return x_hbm.at[:, pl.ds(TWO * t, TWO), pl.ds(core * M, M), :]

    def near(t):
        slot = lax.rem(t, NEAR)
        return pltpu.make_async_copy(half_of(c, t), xl.at[slot], near_sem.at[slot])

    def cross(t):
        slot = lax.rem(t, RING)
        return send(half_of(oc, t), xr.at[slot], xs_sem.at[slot], xr_sem.at[slot], peer)

    loads = [pltpu.make_async_copy(src, fac.at[n], in_sem.at[n])
             for n, src in enumerate((a1_hbm, a2_hbm, a3_hbm, b1_hbm, b2_hbm, b3_hbm))]
    loads.append(pltpu.make_async_copy(d_hbm, d_ref, in_sem.at[len(loads)]))
    for load in loads:
        load.start()
    a1_ref, a2_ref, a3_ref, b1_ref, b2_ref, b3_ref = (fac.at[n] for n in range(len(loads) - 1))
    pl.semaphore_wait(barrier, len(DEVICES))
    for t in range(AHEAD):
        cross(t).start()
    for t in range(NEAR - 1):
        near(t).start()

    for load in loads:
        load.wait()

    def slot_of(dev):
        return QUART * dev[0] + TWO * dev[1] + dev[2]

    dall[slot_of((c, y, z))] = d_ref[...].reshape(H * H, H).T

    def rows_one(p):
        return lax.rem(p // T + H * y, M)

    fill(k1o, a1_ref[...], rows_one, lambda q: c * N + q // T, alike(T))
    fill(k1r, a1_ref[...], rows_one, lambda q: oc * N + q // T, alike(T))

    my_slot = slot_of((c, y, z))

    def diag(rel):
        return send(dall.at[my_slot], dall.at[my_slot], d_sem.at[0], d_sem.at[1], flip(rel))

    for rel in DEVICES:
        diag(rel).start()

    def pack(ref, slot):
        parts = [jnp.concatenate([ref[slot, :, s, 0:T, :], ref[slot, :, s, T:M, :]], axis=-1).reshape(N * T, L)
                 for s in range(TWO)]
        return jnp.concatenate(parts, axis=1)

    def early(t):
        part = (pl.ds(TWO * t, TWO), pl.ds(0, EARLY * T))
        return send(u1s.at[part], u1r.at[part], u1_sem.at[0], u1_sem.at[1], in_x)

    def late(g, n):
        span = N // CHUNKS[g]
        part = (pl.ds(span * n, span), pl.ds(STARTS[g] * T, SIZES[g] * T))
        return send(u1s.at[part], u1r.at[part], late_s, late_r.at[g], in_x)

    @pl.loop(0, STEPS)
    def _(t):
        @pl.when(t + NEAR - 1 < STEPS)
        def _():
            near(t + NEAR - 1).start()

        @pl.when(t >= 1)
        def _():
            early(t - 1).start()

        for n in range(FILLERS):
            @pl.when(t == QUART * (n + 1) + 1)
            def _(n=n):
                late(C, n).start()

        near(t).wait()
        cross(t).wait_recv()
        acc = dot(k1o[...], pack(xl, lax.rem(t, NEAR))) + dot(k1r[...], pack(xr, lax.rem(t, RING)))
        u1 = acc.astype(BF16)
        for s in range(TWO):
            u1o[TWO * t + s] = u1[:H * T, s * L:(s + 1) * L]
            u1s[TWO * t + s] = u1[H * T:, s * L:(s + 1) * L]

        @pl.when(t < STEPS - RING)
        def _():
            pl.semaphore_signal(credit, inc=1, device_id=ids(peer), device_id_type=MESH)

        @pl.when(t + AHEAD >= RING)
        def _():
            cross(t + AHEAD - RING).wait_send()

        @pl.when((t + AHEAD >= RING) & (t + AHEAD < STEPS))
        def _():
            pl.semaphore_wait(credit, 1)

        @pl.when(t + AHEAD < STEPS)
        def _():
            cross(t + AHEAD).start()

    def depart(g, first=0):
        for n in range(first, CHUNKS[g]):
            late(g, n).start()

    early(STEPS - 1).start()
    depart(C, FILLERS)
    depart(D)
    for t in range(STEPS - RING + AHEAD, STEPS):
        cross(t).wait_send()

    fill(k2o, a2_ref[...], lambda p: p // T, lambda q: y * N + q // T, alike(T))
    fill(k2r, a2_ref[...], lambda p: p // T, lambda q: oy * N + q // T, alike(T))
    q = iota((L, N), 1)
    k_first = lax.rem(z + q // T % TWO, TWO) * N + lax.rem(c + q // M, TWO) * M + lax.rem(q, T)
    for half in range(TWO):
        sel = ones_where(iota((L, N), 0) == k_first + T * half)
        k3[half * M:(half + 1) * M, :] = dot(a3_ref[...], sel).astype(BF16)
    fill(l2, b2_ref[...], lambda p: y * N + p // S, lambda q: q // S, alike(S), dot_t)
    fill(l1_out, b1_ref[...], lambda p: c * N + p // S, lambda q: q // S, alike(S), dot_t)
    fill(l3, b3_ref[...], lambda p: z * N + p // L * T + lax.rem(p, T), lambda q: lax.rem(q, M),
         lambda p, q: lax.rem(p, L) // T == q // M, dot_t)

    def second(i, width):
        def side(ref):
            return jnp.concatenate(
                [ref[:, pl.ds(pl.multiple_of((i + s) * T, T), T), :].reshape(N * T, L) for s in range(width)], axis=1)

        own, got = side(u1o), side(u1r)
        part = M * T * width // TWO
        for r0 in range(0, M * T, part):
            out = dot(k2o[r0:r0 + part, :], own) + dot(k2r[r0:r0 + part, :], got)
            for s in range(width):
                u2s[i + s, r0:r0 + part, :] = out[:, s * L:(s + 1) * L].astype(BF16)

    def quarter(dev):
        return TWO * dev[0] + dev[2]

    mine = quarter((c, y, z))

    def inner(g, rel):
        dev = beside(rel)
        i_span = pl.ds(STARTS[g], SIZES[g])
        return send(u2s.at[i_span, pl.ds(quarter(dev) * L, L)], u2b.at[rel - 1, i_span],
                    u2_s, u2_r.at[g], dev)

    def all_second(g):
        if SIZES[g] >= TWO:
            @pl.loop(0, SIZES[g] // TWO)
            def _(n):
                second(STARTS[g] + TWO * n, TWO)
        if SIZES[g] % TWO:
            second(STARTS[g] + SIZES[g] - 1, 1)
        for rel in (1, QUART - 1, TWO):
            inner(g, rel).start()

    low = iota((M, L), 1) < N
    lane = iota((M, TWO * L), 1)

    def third(g):
        got = u2b.at[:, pl.ds(STARTS[g], SIZES[g])]
        send(got, got, u2_s, u2_r.at[g], peer).wait_recv()
        base = slot_of((y, c, 0))
        d = jnp.concatenate([dall[base], dall[base + 1]], axis=0)

        @pl.loop(0, SIZES[g] * QUART, unroll=QUART)
        def _(n):
            i = STARTS[g] + n // QUART
            jl = lax.rem(n, QUART)

            def column(s):
                row = pl.multiple_of((TWO * jl + s) * T, T)
                own = u2s[i, pl.ds(pl.multiple_of(mine * L + row, T), T), :]
                return jnp.concatenate([own] + [u2b[rel - 1, i, pl.ds(row, T), :] for rel in OTHERS], axis=0)

            out = dot(k3[...], jnp.concatenate([column(0), column(1)], axis=1))
            first, other = out[:M], out[M:]
            u3 = jnp.where(low, first[:, :L] + pltpu.roll(other[:, :L], N, 1),
                           pltpu.roll(first[:, L:], N, 1) + other[:, L:])
            at = i * T + S * z + TWO * jl
            even = jnp.sum(jnp.where(lane == at, d, 0.0), axis=1, keepdims=True)
            odd = jnp.sum(jnp.where(lane == at + 1, d, 0.0), axis=1, keepdims=True)
            w = jnp.where(low, even, odd) * u3.astype(BF16).astype(F32)
            wbuf[y * H + i, mine * QUART + jl] = w.astype(BF16)

    def share(g, kind, owner, dev):
        at = (pl.ds(owner[1] * H + STARTS[g], SIZES[g]), pl.ds(quarter(owner) * QUART, QUART))
        return send(wbuf.at[at], wbuf.at[at], w_s, w_r.at[g, BY_KIND[kind]], dev)

    OWN_X, OWN_Y, X_Y, OWN_P, Y_P, X_P, D_P = range(KINDS)
    SAME, OTHER = OWN_P, OWN_P + 1
    BY_KIND = (OWN_X, OWN_Y, X_Y, SAME, SAME, OTHER, OTHER)

    def gather_near(g):
        share(g, OWN_Y, (c, y, z), in_y).start()
        share(g, OWN_P, (c, y, z), peer).start()

    def gather_far(g):
        share(g, OWN_X, (c, y, z), in_x).start()
        if g in DIRECT:
            share(g, X_Y, (c, y, z), diagonal).start()

    def forward_near(g):
        share(g, OWN_Y, in_y, in_y).wait_recv()
        share(g, Y_P, in_y, peer).start()

    def forward_far(g):
        share(g, OWN_X, in_x, in_x).wait_recv()
        if g not in DIRECT:
            share(g, X_Y, in_x, in_y).start()
        share(g, X_P, in_x, peer).start()

    def forward_diagonal(g):
        share(g, X_Y, diagonal, in_y).wait_recv()
        share(g, D_P, diagonal, peer).start()

    def gathered(g, side):
        got = wbuf.at[pl.ds(0, SIZES[g]), pl.ds(0, TWO * QUART)]
        send(got, got, w_s, w_r.at[g, side], peer).wait_recv()

    low_v = iota((QUART, S, S, L), TWO + 1) < N

    def middle(i0):
        for jo in range(TWO):
            rhs = jnp.concatenate(
                [wbuf[i0 + s, jo * S:(jo + 1) * S].reshape(TWO * L, L) for s in range(TWO)], axis=1)
            out = dot(l3[...], rhs)
            for s in range(TWO):
                o = out[:, s * L:(s + 1) * L].reshape(QUART, S, TWO, S, L)
                t0, t1 = o[:, :, 0], o[:, :, 1]
                even = jnp.where(low_v, t0, pltpu.roll(t1, N, TWO + 1))
                odd = jnp.where(low_v, pltpu.roll(t0, N, TWO + 1), t1)
                both = jnp.concatenate([even, odd], axis=TWO).astype(BF16)
                v3[:, s, jo * L:(jo + 1) * L, :] = both.reshape(QUART, L, L)
        for kb in range(QUART):
            out = dot(l2[...], jnp.concatenate([v3[kb, 0], v3[kb, 1]], axis=1))
            pair = jnp.concatenate([out[:, :L].reshape(N, S, L), out[:, L:].reshape(N, S, L)], axis=1)
            v2_out[kb, :, pl.ds(pl.multiple_of(i0 * S, T), T), :] = pair.astype(BF16)

    def near_middle(g):
        for n in range(max(SIZES[g] // TWO, 1)):
            middle(y * H + STARTS[g] + TWO * n)

    def far_middle(g):
        for n in range(max(SIZES[g] // TWO, 1)):
            middle(oy * H + STARTS[g] + TWO * n)

    def near_end(g):
        gathered(g, SAME)

    def far_end(g):
        gathered(g, OTHER)

    def arrived(g):
        got = u1r.at[:, pl.ds(STARTS[g] * T, SIZES[g] * T)]
        send(got, got, late_s, late_r.at[g], in_x).wait_recv()

    first = u1r.at[:, pl.ds(0, EARLY * T)]
    rest = u1r.at[:, pl.ds(EARLY * T, EARLY * T)]
    cores = dall.at[pl.ds(0, len(DEVICES))]
    send(first, first, u1_sem.at[0], u1_sem.at[1], in_x).wait_recv()
    send(cores, cores, d_sem.at[0], d_sem.at[1], peer).wait_recv()
    all_second(A)
    all_second(B)
    arrived(C)
    all_second(C)
    third(A)
    gather_near(A)
    gather_far(A)
    third(B)
    gather_near(B)
    gather_far(B)
    depart(E)
    third(C)
    gather_near(C)
    gather_far(C)
    depart(F)
    depart(G)
    arrived(D)
    all_second(D)
    forward_near(A)
    forward_far(A)
    near_end(A)
    near_middle(A)
    forward_near(B)
    forward_far(B)
    near_end(B)
    near_middle(B)
    forward_near(C)
    third(D)
    gather_near(D)
    gather_far(D)
    forward_diagonal(A)
    far_end(A)
    far_middle(A)
    forward_diagonal(B)
    near_end(C)
    near_middle(C)
    arrived(E)
    all_second(E)
    forward_far(C)
    forward_near(D)
    far_end(B)
    far_middle(B)
    near_end(D)
    near_middle(D)
    arrived(F)
    all_second(F)
    third(E)
    gather_near(E)
    gather_far(E)
    forward_diagonal(C)
    far_end(C)
    far_middle(C)
    third(F)
    gather_near(F)
    gather_far(F)
    arrived(G)
    all_second(G)
    forward_near(E)
    near_end(E)
    near_middle(E)
    forward_far(D)
    forward_near(F)
    forward_far(E)
    third(G)
    gather_near(G)
    gather_far(G)
    forward_diagonal(D)
    forward_far(F)
    forward_diagonal(E)
    far_end(D)
    far_middle(D)
    forward_near(G)
    forward_diagonal(F)
    forward_far(G)
    forward_diagonal(G)
    near_end(F)
    near_end(G)
    near_middle(F)
    far_end(E)
    far_middle(E)
    far_end(F)
    far_end(G)
    far_middle(F)

    sent = wbuf.at[pl.ds(0, KINDS * QUART), :]
    send(first, first, u1_sem.at[0], u1_sem.at[1], in_x).wait_send()
    send(rest, rest, late_s, late_r.at[0], in_x).wait_send()
    send(cores, cores, d_sem.at[0], d_sem.at[1], peer).wait_send()
    send(u2b, u2b, u2_s, u2_r.at[0], peer).wait_send()
    send(sent, sent, w_s, w_r.at[0, 0], peer).wait_send()


def compress(x, a1, a2, a3, b1_t, b2_t, b3_t, d):
    vmem = pl.BlockSpec(memory_space=pltpu.VMEM)
    hbm = pl.BlockSpec(memory_space=pltpu.HBM)
    dma = pltpu.SemaphoreType.DMA
    u1 = pltpu.VMEM((N, H * T, L), BF16)
    spread = pltpu.VMEM((M * T, N * T), BF16)
    groups = len(SIZES)
    return pl.pallas_call(
        compress_body,
        out_shape=(pltpu.VMEM((QUART, N, M * S, L), BF16), pltpu.VMEM((N * S, M * S), BF16)),
        in_specs=[hbm] * 8,
        out_specs=(vmem, vmem),
        scratch_shapes=[
            pltpu.VMEM((6, M, L), BF16), pltpu.VMEM((H, H, H), F32),
            pltpu.VMEM((NEAR, N, TWO, M, N), BF16), pltpu.VMEM((RING, N, TWO, M, N), BF16), u1, u1, u1,
            spread, spread, spread, spread, pltpu.VMEM((N, N), BF16),
            pltpu.VMEM((M * T, M * S), BF16), pltpu.VMEM((N * S, M * S), BF16),
            pltpu.VMEM((H, M * T, L), BF16), pltpu.VMEM((len(OTHERS), H, L, L), BF16),
            pltpu.VMEM((M, H, M, L), BF16), pltpu.VMEM((S, H, H * H), F32),
            pltpu.VMEM((QUART, TWO, M * S, L), BF16),
            dma((NEAR,)), dma((RING,)), dma((RING,)), pltpu.SemaphoreType.REGULAR,
            dma((TWO,)), dma, dma((groups,)), dma, dma((groups,)), dma, dma((groups, QUART + 1)), dma((TWO,)), dma((KINDS,)),
        ],
        compiler_params=pltpu.CompilerParams(collective_id=0, has_side_effects=True, vmem_limit_bytes=LIMIT),
        name="compress",
    )(x, a1, a2, a3, b1_t, b2_t, b3_t, d)


def expand_body(v2_ref, l1_ref, z_hbm, zbuf, z_sem):
    per_block = N // COLUMNS

    def leave(n):
        slot = lax.rem(n, SLOTS)
        where = (slice(None), pl.ds(n % per_block * COLUMNS, COLUMNS), pl.ds(n // per_block * T, T))
        return pltpu.make_async_copy(zbuf.at[slot], z_hbm.at[where], z_sem.at[slot])

    @pl.loop(0, QUART * per_block)
    def _(n):
        slot = lax.rem(n, SLOTS)

        @pl.when(n >= SLOTS)
        def _():
            leave(n - SLOTS).wait()

        for j in range(0, COLUMNS, TWO):
            at = n % per_block * COLUMNS + j
            out = dot(l1_ref[...], jnp.concatenate([v2_ref[n // per_block, at + s] for s in range(TWO)], axis=1))
            for s in range(TWO):
                o = out[:, s * L:(s + 1) * L].reshape(N, S, L)
                zbuf[slot, :, j + s, :S, :] = o[:, :, :N]
                zbuf[slot, :, j + s, S:, :] = pltpu.roll(o, N, TWO)[:, :, :N]
        leave(n).start()

    for n in range(QUART * per_block - SLOTS, QUART * per_block):
        leave(n).wait()


def expand(v2, l1):
    vmem = pl.BlockSpec(memory_space=pltpu.VMEM)
    return pl.pallas_call(
        expand_body,
        out_shape=jax.ShapeDtypeStruct((N, N, N, N), F32),
        in_specs=[vmem, vmem],
        out_specs=pl.BlockSpec(memory_space=pl.ANY),
        scratch_shapes=[pltpu.VMEM((SLOTS, N, COLUMNS, T, N), F32), pltpu.SemaphoreType.DMA((SLOTS,))],
        compiler_params=pltpu.CompilerParams(vmem_limit_bytes=LIMIT // 2),
        name="expand",
    )(v2, l1)


def solution(mesh):
    vol_spec = P("mx", "my", "mz", "rhs")
    core_spec = P("mx", "my", "mz")
    full_spec = P()

    def local_operator(x_blk, fac_a1, fac_a2, fac_a3, diag_blk, fac_b1, fac_b2, fac_b3):
        v2, l1 = compress(x_blk, fac_a1, fac_a2, fac_a3, fac_b1.T, fac_b2.T, fac_b3.T, diag_blk)
        return expand(v2, l1)

    return jax.shard_map(local_operator, mesh=mesh, in_specs=(vol_spec, full_spec, full_spec, full_spec, core_spec, full_spec, full_spec, full_spec), out_specs=vol_spec, check_vma=False)
```
